32 devices in a mesh: gx: 4 (over z), gy: 8 (over y, x, core).
Axes of the slice: x: 2, y: 2, z: 4, core: 2. Of those that a mesh axis runs over, the one named last changes fastest.
Arguments:
- populations: float32 [19, 64, 32, 128], P(None, 'gx', 'gy'), as said below
- vert_base: int32 [3, 16384], P(None, ('gx', 'gy')), may hold values from 0 to 127, as said below
- vert_frac: float32 [3, 16384], P(None, ('gx', 'gy')), may hold values from 0 to 0.999
- edges: int32 [2, 49152], P(None, ('gx', 'gy')), may hold values from 0 to 511, as said below
- stiffness: float32 [49152], P(('gx', 'gy')), may hold values from 0.05 to 0.5
- rest: float32 [3, 49152], P(None, ('gx', 'gy')), may hold values from -3 to 3
Outputs:
- fresh: float32 [19, 64, 32, 128], P(None, 'gx', 'gy')
- vertex_velocity: float32 [3, 16384], P(None, ('gx', 'gy'))
The draws below stay inside these ranges and needn't reach their ends.
Inputs may be any that keep to these rules, and one draw needn't show every extreme that they name: `vert_base`: the first coordinate lies below 64, the second below 32, the third below 128. The vertices are in blocks of 512, block k belonging to the k-th device in the order gx then gy; a vertex's first coordinate lies in that device's 16 cells along x, its second in its 4 cells along y. Each run of 128 vertices of a block lies in a box of 4 x 4 x 4 cells, periodic in z. `edges`: edge e belongs to block e // 1536; its two entries are distinct indices within that block's 512 vertices, both in the same run of 128 vertices. `populations`: every entry lies between 0.6 and 1.4 times the lattice weight of its direction.
All inputs are finite; a program needn't handle non-finite values.
Results may differ from the reference program's by a relative error of at most 0.000078.
Values sent between devices are 32-bit elements; how exact they have to be, the bound alone decides.
A program may use at most 64 MiB of HBM per device.

```python
import math
import jax
import jax.numpy as jnp
import numpy as np
from jax import lax

CX = 16
CY = 4
NZ = 128
VERT_DEV = 512
TILE = 128
NX = 64
NY = 32
VERTS = 16384
EDGE_DEV = 1536
EDGES = 49152


table_weights = np.array([1.0 / 3.0] + [1.0 / 18.0] * 6 + [1.0 / 36.0] * 12, np.float32)


def draw_populations(key, part):
    shape = (19, NX, NY, NZ)
    noise = jax.random.uniform(key, shape, jnp.float32, -0.38, 0.38)
    weights = jnp.asarray(table_weights, jnp.float32)[:, None, None, None]
    return weights * (1.0 + noise)


def draw_vert_base(key, part):
    tile_count = VERTS // TILE
    column_count = NY // CY
    vertex = jnp.arange(VERTS, dtype=jnp.int32)
    block = vertex // VERT_DEV
    tile = vertex // TILE
    tile_x = jax.random.randint(jax.random.fold_in(key, 11), (tile_count,), 0, CX - 3)
    tile_y = jax.random.randint(jax.random.fold_in(key, 12), (tile_count,), 0, CY - 3)
    tile_z = jax.random.randint(jax.random.fold_in(key, 13), (tile_count,), 0, NZ)
    spread = jax.random.randint(jax.random.fold_in(key, 14), (3, VERTS), 0, 4)
    first = block // column_count * CX + tile_x[tile] + spread[0]
    second = block % column_count * CY + tile_y[tile] + spread[1]
    third = (tile_z[tile] + spread[2]) % NZ
    return jnp.stack([first, second, third]).astype(jnp.int32)


def draw_edges(key, part):
    local = jnp.arange(EDGES, dtype=jnp.int32) % EDGE_DEV
    group = local // (3 * TILE)
    start = jax.random.randint(jax.random.fold_in(key, 21), (EDGES,), 0, TILE)
    stride = jax.random.randint(jax.random.fold_in(key, 22), (EDGES,), 1, TILE)
    first = group * TILE + start
    second = group * TILE + (start + stride) % TILE
    return jnp.stack([first, second]).astype(jnp.int32)


def levels(rng, extent, pieces, smallest, largest):
    gain = 1.0
    for dim, shards_of in pieces:
        steps = jax.random.uniform(jax.random.fold_in(jax.random.fold_in(rng, 6), dim), (shards_of,), jnp.float32, smallest / len(pieces), largest / len(pieces))
        gain = gain * jnp.repeat(jnp.exp(steps), extent[dim] // shards_of).reshape((-1,) + (1,) * (len(extent) - 1 - dim))
    return gain


def centred(stream_key, shape, scale, most, pieces=(), kind=jnp.bfloat16):
    factor_of = levels(stream_key, shape, pieces, -0.22, 0.18) if pieces else 1.0
    drawn = jax.random.normal(stream_key, shape, jnp.float32) * scale * factor_of
    return jnp.minimum(jnp.maximum(drawn, -most), most).astype(kind)


def setup_inputs(seed: int = 0) -> dict:
    streams_of = jax.random.split(jax.random.key(seed), 7)
    return {
        "populations": draw_populations(jax.random.fold_in(streams_of[6], 71), 0),
        "vert_base": draw_vert_base(jax.random.fold_in(streams_of[6], 71), 0),
        "vert_frac": jnp.clip(0.999 * jax.random.uniform(streams_of[2], (3, VERTS), jnp.float32) ** levels(streams_of[2], (3, VERTS), ((1, 32),), -0.2, 0.2), 0.0, 0.999),
        "edges": draw_edges(jax.random.fold_in(streams_of[6], 71), 0),
        "stiffness": jnp.clip(jnp.exp(math.log(0.5) - 2.3025851 * jax.random.uniform(streams_of[4], (EDGES,), jnp.float32) ** levels(streams_of[4], (EDGES,), ((0, 32),), -0.2, 0.2)), 0.05, 0.5),
        "rest": centred(streams_of[5], (3, EDGES), 0.5, 3.0, ((1, 32),), jnp.float32),
    }


lattice_speeds = [(0, 0, 0), (1, 0, 0), (-1, 0, 0), (0, 1, 0), (0, -1, 0), (0, 0, 1), (0, 0, -1), (1, 1, 0), (-1, -1, 0), (1, -1, 0), (-1, 1, 0), (1, 0, 1), (-1, 0, -1), (1, 0, -1), (-1, 0, 1), (0, 1, 1), (0, -1, -1), (0, 1, -1), (0, -1, 1)]
lattice_weights = [1.0 / 3.0] + [1.0 / 18.0] * 6 + [1.0 / 36.0] * 12
relax_time = 0.9

def outer_weight(r):
    return (5.0 - 2.0 * r - jnp.sqrt(-7.0 + 12.0 * r - 4.0 * r * r)) / 8.0

def inner_weight(r):
    return (3.0 - 2.0 * r + jnp.sqrt(1.0 + 4.0 * r - 4.0 * r * r)) / 8.0

def kernel_weights(frac):
    return jnp.stack([outer_weight(1.0 + frac), inner_weight(frac), inner_weight(1.0 - frac), outer_weight(2.0 - frac)])

def collide(popul, force):
    speeds = jnp.asarray(lattice_speeds, jnp.float32)
    weights = jnp.asarray(lattice_weights, jnp.float32)[:, None, None, None]
    high = lax.Precision.HIGHEST
    density = lax.optimization_barrier(jnp.sum(popul, axis=0))
    moment = jnp.tensordot(speeds.T, popul, axes=1, precision=high)
    velocity = (moment + 0.5 * force) / density
    along = jnp.tensordot(speeds, velocity, axes=1, precision=high)
    square = lax.optimization_barrier(jnp.sum(velocity * velocity, axis=0))
    balance = weights * density * (1.0 + 3.0 * along + 4.5 * along * along - 1.5 * square)
    push = jnp.tensordot(speeds, force, axes=1, precision=high)
    work = lax.optimization_barrier(jnp.sum(velocity * force, axis=0))
    source = (1.0 - 0.5 / relax_time) * weights * (3.0 * (push - work) + 9.0 * along * push)
    post = popul - (popul - balance) / relax_time + source
    return (post, velocity)

def reference(populations, vert_base, vert_frac, edges, stiffness, rest):
    position = vert_base.astype(jnp.float32) + vert_frac
    offset = jnp.arange(EDGES, dtype=jnp.int32) // EDGE_DEV * VERT_DEV
    first = edges[0] + offset
    second = edges[1] + offset
    stretch = stiffness[None, :] * (position[:, second] - position[:, first] - rest)
    membrane = jnp.zeros((3, VERTS), jnp.float32).at[:, first].add(stretch).at[:, second].add(-stretch)
    kernel = kernel_weights(vert_frac)
    grid = jnp.zeros((3, NX, NY, NZ), jnp.float32)
    cells = []
    for kx in range(4):
        for ky in range(4):
            for kz in range(4):
                index_x = (vert_base[0] - 1 + kx) % NX
                index_y = (vert_base[1] - 1 + ky) % NY
                index_z = (vert_base[2] - 1 + kz) % NZ
                weight = kernel[kx, 0] * kernel[ky, 1] * kernel[kz, 2]
                cells.append((index_x, index_y, index_z, weight))
                grid = grid.at[:, index_x, index_y, index_z].add(membrane * weight[None, :])
    post, velocity = collide(populations, grid)
    rows = []
    for q in range(19):
        shift = lattice_speeds[q]
        rows.append(jnp.roll(post[q], shift, axis=(0, 1, 2)))
    fresh = jnp.stack(rows)
    sampled = jnp.zeros((3, VERTS), jnp.float32)
    for index_x, index_y, index_z, weight in cells:
        sampled = sampled + velocity[:, index_x, index_y, index_z] * weight[None, :]
    return (fresh, sampled)
```

```python
import jax
import jax.numpy as jnp
from jax import lax
from jax.experimental import pallas as pl
from jax.experimental.pallas import tpu as pltpu
from jax.sharding import PartitionSpec as P

lattice_speeds = [
    (0, 0, 0),
    (1, 0, 0),
    (-1, 0, 0),
    (0, 1, 0),
    (0, -1, 0),
    (0, 0, 1),
    (0, 0, -1),
    (1, 1, 0),
    (-1, -1, 0),
    (1, -1, 0),
    (-1, 1, 0),
    (1, 0, 1),
    (-1, 0, -1),
    (1, 0, -1),
    (-1, 0, 1),
    (0, 1, 1),
    (0, -1, -1),
    (0, 1, -1),
    (0, -1, 1),
]
lattice_weights = [1.0 / 3.0] + [1.0 / 18.0] * 6 + [1.0 / 36.0] * 12
relax_time = 0.9
run = 128
window = 8
sides = [(1, 1), (1, -1), (-1, 1), (-1, -1), (0, 1), (0, -1), (1, 0), (-1, 0)]
groups = [(0, 1, 6), (2, 3, 7), (4,), (5,)]
f32, bf16 = jnp.float32, jnp.bfloat16


def outer_weight(r):
    return (5.0 - 2.0 * r - jnp.sqrt(-7.0 + 12.0 * r - 4.0 * r * r)) / 8.0


def inner_weight(r):
    return (3.0 - 2.0 * r + jnp.sqrt(1.0 + 4.0 * r - 4.0 * r * r)) / 8.0


def up(n, m):
    return (n + m - 1) // m * m


class Plan:
    def __init__(self, wx, wy):
        self.wx, self.wy, self.own = wx, wy, wx * wy
        self.h = up(wy + 3, 8)
        self.cols = wx + 3
        self.rows = up(self.cols * self.h, 16)
        self.xs = list(range(-1, wx + 2))

        def span(d, w):
            return {0: list(range(-1, w + 2)), 1: [w - 1, w, w + 1], -1: [-1, 0, 1]}[d]

        def edge(d, w):
            return {0: list(range(w)), 1: [w - 1], -1: [0, 1]}[d]

        def near(d, w):
            return {0: list(range(w)), 1: [w - 1], -1: [0]}[d]

        def cells(d, pick):
            xs, ys = pick(d[0], wx), pick(d[1], wy)
            if d[0]:
                return [(x, y) for x in xs for y in ys]
            return [(x, y) for y in ys for x in xs]

        self.edge = [cells(d, edge) for d in sides]
        self.near = [cells(d, near) for d in sides]
        self.force = [cells(d, span) for d in sides]
        self.dirs = [
            [
                q
                for q, c in enumerate(lattice_speeds)
                if (not d[0] or c[0] == d[0]) and (not d[1] or c[1] == d[1])
            ]
            for d in sides
        ]
        self.macro_rows = [
            4 * len(e) + len(q) * len(n) + 1 for e, q, n in zip(self.edge, self.dirs, self.near)
        ]
        self.force_rows = [3 * self.h if d[1] == 0 else len(c) for d, c in zip(sides, self.force)]

    def row(self, x, y):
        return (x + 1) * self.h + y % self.h

    def there(self, cell, d):
        return self.row(cell[0] - d[0] * self.wx, cell[1] - d[1] * self.wy)

    def late(self, x):
        return x < 2 or x > self.wx - 2


def runs(src, dst):
    out, i = [], 0
    while i < len(src):
        n, a, b = 1, 1, 1
        if i + 1 < len(src) and src[i + 1] > src[i] and dst[i + 1] > dst[i]:
            a, b = src[i + 1] - src[i], dst[i + 1] - dst[i]
            n = 2
            while i + n < len(src) and src[i + n] - src[i + n - 1] == a and dst[i + n] - dst[i + n - 1] == b:
                n += 1
        out.append((src[i], a, dst[i], b, n))
        i += n
    return out


def ds(start, n, stride):
    return pl.ds(start, n, stride=stride) if stride > 1 else pl.ds(start, n)


def move(src_ref, src, dst_ref, dst):
    for s, a, d, b, n in runs(src, dst):
        dst_ref[ds(d, n, b), :] = src_ref[ds(s, n, a), :]


def split(value):
    high = value.astype(bf16)
    return high, (value - high.astype(f32)).astype(bf16)


def halves(value):
    return jnp.concatenate(split(value), axis=0)


def pick4(delta, weights):
    out = jnp.zeros(delta.shape, f32)
    for k in range(4):
        out = jnp.where(delta == k, weights[k], out)
    return out


def wrap(value, depth):
    value = jnp.where(value < 0, value + depth, value)
    return jnp.where(value >= depth, value - depth, value)


def along_speed(c, vector):
    total = None
    for k in range(3):
        if c[k]:
            term = vector[k] if c[k] > 0 else -vector[k]
            total = term if total is None else total + term
    return total


def transposed_dot(a, b):
    return lax.dot_general(a, b, (((1,), (1,)), ((), ())), preferred_element_type=f32)


def exchange_kernel(plan, nx, ny, *refs):
    wx, wy, h, rows, own = plan.wx, plan.wy, plan.h, plan.rows, plan.own
    sources, results, scratch = refs[0:6], refs[6:10], refs[10:]
    fresh, vel, plane, along = results
    ms, mr, fs, fr = scratch[0:8], scratch[8:16], scratch[16:24], scratch[24:32]
    (pops, base, frac, edges, stiff, rest, pos, pull, mem, mac, grid, comb, px_ref) = scratch[32:45]
    placed = scratch[45:53]
    ones_y, ones_l, ones_r, edge_pops, sems, load_sems, ready = scratch[53:]
    depth = pops.shape[1]
    load_into = (pops.at[pl.ds(0, 19 * own), :], base, frac, edges, stiff, rest)
    loads_in = [pltpu.make_async_copy(sources[n], load_into[n], load_sems.at[n]) for n in range(6)]
    for n in (3, 2, 1, 5, 4, 0):
        loads_in[n].start()
    count = base.shape[1]
    edge_count = edges.shape[1]
    tiles = count // run
    ix, iy = lax.axis_index("gx"), lax.axis_index("gy")
    peers = [(lax.rem(ix + dx + nx, nx), lax.rem(iy + dy + ny, ny)) for dx, dy in sides]
    key = ix * ny + iy
    lead = [(key < peers[g[0]][0] * ny + peers[g[0]][1]).astype(jnp.int32) for g in groups]
    barrier = pltpu.get_barrier_semaphore()

    def hail(sem, n):
        pl.semaphore_signal(sem, inc=1, device_id=peers[n], device_id_type=pl.DeviceIdType.MESH)

    for i, g in enumerate(groups):

        @pl.when(lead[i] == 1)
        def _():
            for n in g:
                hail(barrier, n)

    greetings = sum((1 - lead[i]) * len(g) for i, g in enumerate(groups))

    @pl.when(greetings > 0)
    def _():
        pl.semaphore_wait(barrier, greetings)

    for i, g in enumerate(groups):

        @pl.when(lead[i] == 0)
        def _():
            for n in g:
                hail(ready.at[sides.index((-sides[n][0], -sides[n][1]))], n)

    def copies(src, dst, kind):
        return [
            pltpu.make_async_remote_copy(
                src_ref=src[n],
                dst_ref=dst[n],
                send_sem=sems.at[kind, n],
                recv_sem=sems.at[kind + 1, n],
                device_id=peers[n],
                device_id_type=pl.DeviceIdType.MESH,
            )
            for n in range(8)
        ]

    first_col = {1: wx, -1: 0}
    outgoing = list(fs)
    for n in (6, 7):
        outgoing[n] = comb.at[pl.ds(first_col[sides[n][0]] * h, 3 * h), :]
    macro_copies = copies(ms, mr, 0)
    force_copies = copies(outgoing, fr, 2)

    zeros = jnp.zeros((8, run), f32)
    pos[...] = jnp.zeros(pos.shape, f32)
    pull[...] = jnp.zeros(pull.shape, f32)
    for ref in placed:
        ref[...] = jnp.zeros(ref.shape, f32)
    for n in (3, 2, 1, 5, 4):
        loads_in[n].wait()

    moved = frac[...]
    weights = [
        outer_weight(1.0 + moved),
        inner_weight(moved),
        inner_weight(1.0 - moved),
        outer_weight(2.0 - moved),
    ]
    lane = lax.broadcasted_iota(jnp.int32, (1, run), 1)
    slot = lax.rem(lane, window)
    of_tile = lax.rem(lane // window, tiles)
    start_of = jnp.zeros((1, run), jnp.int32)
    offsets = []
    for t in range(tiles):
        z = base[2:3, t * run : (t + 1) * run]
        gap = z - z[0:1, 0:1]
        gap = jnp.where(gap > depth // 2, gap - depth, gap)
        gap = jnp.where(gap < -(depth // 2), gap + depth, gap)
        low = jnp.min(gap, axis=1, keepdims=True)
        offsets.append(gap - low)
        start_of = jnp.where(of_tile == t, z[0:1, 0:1] + low - 1, start_of)
    zmap = wrap(start_of + slot, depth).astype(f32)
    offset = jnp.concatenate(offsets, axis=1)
    reach_z = pick4(lax.broadcasted_iota(jnp.int32, (window, count), 0) - offset, [w[2:3] for w in weights])

    loads_in[0].wait()
    for r in range(0, own, 8):
        totals = [None] * 4
        for q, c in enumerate(lattice_speeds):
            value = pops[pl.ds(q * own + r, 8), :]
            for k, sign in enumerate((1,) + c):
                if sign:
                    term = value if sign > 0 else -value
                    totals[k] = term if totals[k] is None else totals[k] + term
        for k in range(4):
            for i in range(0, 8, wy):
                mac[pl.ds(k * rows + plan.row((r + i) // wy, 0), wy), :] = totals[k][i : i + wy]
    for n in range(8):
        cells, close = plan.edge[n], plan.near[n]
        for k in range(4):
            move(
                mac,
                [k * rows + plan.row(x, y) for x, y in cells],
                ms[n],
                [k * len(cells) + i for i in range(len(cells))],
            )
        for s, q in enumerate(plan.dirs[n]):
            first = 4 * len(cells) + s * len(close)
            move(pops, [q * own + x * wy + y for x, y in close], ms[n], [first + i for i in range(len(close))])
        ms[n][pl.ds(plan.macro_rows[n] - 1, 1), :] = zmap
    for i, g in enumerate(groups):

        @pl.when(lead[i] == 0)
        def _():
            for n in g:
                macro_copies[n].start()

    part = 8 * tiles
    high = moved.astype(bf16).astype(f32)
    low = moved - high
    whole = base[...].astype(f32)
    for t in range(tiles):
        cols = slice(t * run, (t + 1) * run)
        pos[pl.ds(8 * t, 3), :] = whole[:, cols]
        pos[pl.ds(part + 8 * t, 3), :] = high[:, cols]
        pos[pl.ds(2 * part + 8 * t, 3), :] = low[:, cols]
    ends = edges[...]
    spot = lax.broadcasted_iota(jnp.int32, (run, edge_count), 0)
    tail = jnp.bitwise_and(ends[0:1], run - 1)
    head = jnp.bitwise_and(ends[1:2], run - 1)
    hot = jnp.where(spot == head, 1.0, jnp.where(spot == tail, -1.0, 0.0)).astype(bf16)
    group = lax.shift_right_logical(ends[0:1], run.bit_length() - 1)
    reach = jnp.dot(pos[...].astype(bf16), hot, preferred_element_type=f32)
    reach = reach[0:part] + reach[part : 2 * part] + reach[2 * part : 3 * part]
    pull[pl.ds(0, 3), :] = rest[...]
    diff = jnp.zeros((8, edge_count), f32)
    for t in range(tiles):
        diff = jnp.where(group == t, reach[8 * t : 8 * t + 8], diff)
    stretch = stiff[...].reshape(1, edge_count) * (diff - pull[...])
    terms = jnp.concatenate([jnp.where(group == t, stretch, 0.0) for t in range(tiles)], axis=0)
    summed = transposed_dot(halves(terms), hot)
    summed = summed[0:part] + summed[part : 2 * part]
    for t in range(tiles):
        mem[:, t * run : (t + 1) * run] = -summed[8 * t : 8 * t + 8]

    bx = base[0:1, :] - ix * wx - 1
    by = base[1:2, :] - iy * wy - 1
    i = lax.broadcasted_iota(jnp.int32, (px_ref.shape[0], 1), 0)
    px_ref[...] = pick4(i - 1 - bx, [w[0:1] for w in weights])
    i = lax.broadcasted_iota(jnp.int32, (h, 1), 0)
    y = jnp.where(i == h - 1, -1, jnp.where(i > wy + 1, -100, i))
    py = pick4(y - by, [w[1:2] for w in weights])
    for k in range(rows // h):
        if k < plan.cols:
            plane[pl.ds(k * h, h), :] = px_ref[pl.ds(k, 1), :] * py
        else:
            plane[pl.ds(k * h, h), :] = jnp.zeros((h, count), f32)

    big, small = [], []
    for c in range(3):
        for t in range(tiles):
            cols = slice(t * run, (t + 1) * run)
            block = reach_z[:, cols] * mem[c : c + 1, cols]
            rounded = block.astype(bf16).astype(f32)
            for out, value in ((big, rounded), (small, block - rounded)):
                out.append(jnp.concatenate([value if t == s else zeros for s in range(tiles)], axis=1))
    pad = [jnp.zeros((run - 3 * tiles * window, count), f32)]
    spread = transposed_dot(halves(plane[...]), jnp.concatenate(big + pad + small + pad, axis=0).astype(bf16))
    spread = spread[0:rows] + spread[rows : 2 * rows]
    comb[...] = spread[:, 0:run] + spread[:, run : 2 * run]
    for n in range(6):
        move(comb, [plan.row(x, y) for x, y in plan.force[n]], fs[n], list(range(plan.force_rows[n])))
    for i, g in enumerate(groups):

        @pl.when(lead[i] == 0)
        def _():
            for n in g:
                force_copies[n].start()

    for i in (2, 3, 0, 1):

        @pl.when(lead[i] == 1)
        def _():
            for n in groups[i]:
                pl.semaphore_wait(ready.at[n], 1)
                macro_copies[n].start()
                force_copies[n].start()

    gap = wrap(lax.broadcasted_iota(jnp.int32, (depth, count), 0) - (base[2:3, :] - 1), depth)
    z_high, z_low = split(pick4(gap, [w[2:3] for w in weights]))
    along[pl.ds(0, depth), :] = z_high
    along[pl.ds(depth, depth), :] = z_low

    comp_of = lane // (window * tiles)

    def mark(ones, s, zrow):
        at = jnp.where(lax.broadcasted_iota(jnp.int32, (depth, run), 0).astype(f32) == zrow, 1.0, 0.0)
        for c in range(3):
            ones[pl.ds(c * depth, depth), pl.ds(s * run, run)] = jnp.where(comp_of == c, at, 0.0).astype(bf16)

    def take_macro(n):
        macro_copies[n].wait_recv()
        cells, close, d = plan.edge[n], plan.near[n], sides[n]
        for k in range(4):
            move(
                mr[n],
                [k * len(cells) + i for i in range(len(cells))],
                mac,
                [k * rows + plan.there(c, d) for c in cells],
            )
        return mr[n][pl.ds(plan.macro_rows[n] - 1, 1), :]

    def pop_row(n, q, cell):
        cells, close = plan.edge[n], plan.near[n]
        return 4 * len(cells) + plan.dirs[n].index(q) * len(close) + close.index(cell)

    keep = 1.0 - 1.0 / relax_time
    half = 1.0 - 0.5 / relax_time
    level_row = lax.broadcasted_iota(jnp.int32, (h, 1), 0)

    def population(q, x):
        c = lattice_speeds[q]
        if x < 0 or x >= wx:
            return edge_pops[pl.ds(q * h, h), :]
        value = pops[pl.ds(q * own + x * wy, h), :]
        if c[1] == 1:
            value = jnp.where(level_row == h - 1, mr[4][pl.ds(pop_row(4, q, (x, wy - 1)), 1), :], value)
        if c[1] == -1:
            value = jnp.where(level_row == wy, mr[5][pl.ds(pop_row(5, q, (x, 0)), 1), :], value)
        return value

    def collide(x):
        at = (x + 1) * h
        density = mac[pl.ds(at, h), :]
        force = [grid[pl.ds(k * rows + at, h), :] for k in range(3)]
        inverse = 1.0 / density
        speed = [(mac[pl.ds((k + 1) * rows + at, h), :] + 0.5 * force[k]) * inverse for k in range(3)]
        for k in range(3):
            vel[pl.ds(k * rows + at, h), :] = jnp.where((level_row <= wy + 1) | (level_row == h - 1), speed[k], 0.0)
        square = speed[0] * speed[0] + speed[1] * speed[1] + speed[2] * speed[2]
        work = speed[0] * force[0] + speed[1] * force[1] + speed[2] * force[2]
        scaled = density * (1.0 / relax_time)
        level = scaled * (1.0 - 1.5 * square) - (3.0 * half) * work
        for first in [0] + list(range(1, 19, 2)):
            pair = [0] if first == 0 else [first, first + 1]
            pair = [q for q in pair if 0 <= x + lattice_speeds[q][0] < wx]
            if not pair:
                continue
            weight = lattice_weights[first]
            if first == 0:
                even, odd = level * weight, None
            else:
                a = along_speed(lattice_speeds[first], speed)
                push = along_speed(lattice_speeds[first], force)
                turn = scaled * a + half * push
                even = weight * (level + a * (4.5 * scaled * a + 9.0 * half * push))
                odd = (3.0 * weight) * turn
            for q in pair:
                c = lattice_speeds[q]
                value = keep * population(q, x) + even
                if odd is not None:
                    value = value + odd if q == first else value - odd
                if c[1]:
                    value = pltpu.roll(value, c[1] % h, 0)
                if c[2]:
                    value = pltpu.roll(value, c[2] % depth, 1)
                fresh[pl.ds(q * own + (x + c[0]) * wy, wy), :] = value[0:wy]

    mark(ones_y, 0, zmap)
    for s, n in ((1, 4), (2, 5)):
        mark(ones_y, s, take_macro(n))
    for n in (4, 5):
        force_copies[n].wait_recv()
        move(fr[n], list(range(plan.force_rows[n])), placed[n], [plan.there(c, sides[n]) for c in plan.force[n]])

    def widen(parts, ones):
        value = transposed_dot(halves(jnp.concatenate(parts, axis=1)), ones[...])
        half_rows = value.shape[0] // 2
        return value[0:half_rows] + value[half_rows:]

    value = widen([comb[...], placed[4][...], placed[5][...]], ones_y)
    for c in range(3):
        grid[pl.ds(c * rows, rows), :] = value[:, c * depth : (c + 1) * depth]
    for x in plan.xs:
        if not plan.late(x):
            collide(x)

    edge_rows = {-1: 6, 1: 7}
    for ones, order in ((ones_l, (6, 0, 1)), (ones_r, (7, 2, 3))):
        for s, n in enumerate(order):
            mark(ones, s, take_macro(n))
            for q in plan.dirs[n]:
                for s_cell in plan.near[n]:
                    pass
                close = plan.near[n]
                src = [pop_row(n, q, c) for c in close]
                dst = [q * h + (c[1] - sides[n][1] * wy) % h for c in close]
                move(mr[n], src, edge_pops, dst)
    for ones, order in ((ones_l, (6, 0, 1)), (ones_r, (7, 2, 3))):
        for n in order:
            force_copies[n].wait_recv()
            if n < 4:
                at = 0 if sides[n][0] == 1 else wx * h
                dst = [plan.there(c, sides[n]) - at for c in plan.force[n]]
                move(fr[n], list(range(plan.force_rows[n])), placed[n], dst)
        value = widen([fr[order[0]][...], placed[order[1]][...], placed[order[2]][...]], ones)
        at = 0 if ones is ones_l else wx * h
        for c in range(3):
            here = pl.ds(c * rows + at, 3 * h)
            grid[here, :] = grid[here, :] + value[:, c * depth : (c + 1) * depth]
    for x in plan.xs:
        if plan.late(x):
            collide(x)
    spare = rows - plan.cols * h
    if spare:
        for k in range(3):
            vel[pl.ds(k * rows + plan.cols * h, spare), :] = jnp.zeros((spare, depth), f32)

    for copy in macro_copies + force_copies:
        copy.wait_send()


def finish_kernel(plan, fresh, vel, plane, along, fresh_out, sampled_out, sampled, sems):
    rows, own = plan.rows, plan.own
    depth = fresh.shape[1]
    pieces = [list(range(19))[i::4] for i in range(4)]
    cuts = [0, 5, 10, 15, 19]
    leave = [
        pltpu.make_async_copy(
            fresh.at[pl.ds(a * own, (b - a) * own), :], fresh_out.at[pl.ds(a * own, (b - a) * own), :], sems.at[i]
        )
        for i, (a, b) in enumerate(zip(cuts, cuts[1:]))
    ]
    for copy in leave:
        copy.start()
    last = pltpu.make_async_copy(sampled, sampled_out, sems.at[4])
    v_high, v_low = split(vel[...])
    value = jnp.dot(v_high, along[pl.ds(0, depth), :], preferred_element_type=f32)
    value = value + jnp.dot(v_low, along[pl.ds(0, depth), :], preferred_element_type=f32)
    value = value + jnp.dot(v_high, along[pl.ds(depth, depth), :], preferred_element_type=f32)
    flat = plane[...]
    for k in range(3):
        sampled[k : k + 1, :] = jnp.sum(value[k * rows : (k + 1) * rows] * flat, axis=0, keepdims=True)
    last.start()
    for copy in leave + [last]:
        copy.wait()


def solution(mesh):
    nx, ny = mesh.shape["gx"], mesh.shape["gy"]

    def per_device(populations, vert_base, vert_frac, edges, stiffness, rest):
        _, wx, wy, depth = populations.shape
        count, edge_count = vert_base.shape[1], edges.shape[1]
        plan = Plan(wx, wy)
        rows, tiles, h = plan.rows, count // run, plan.h
        macro = [pltpu.VMEM((n, depth), f32) for n in plan.macro_rows]
        force = [pltpu.VMEM((n, run), f32) for n in plan.force_rows]
        scratch = macro + macro + force + force
        scratch += [
            pltpu.VMEM((19 * wx * wy + h, depth), f32),
            pltpu.VMEM((3, count), jnp.int32),
            pltpu.VMEM((3, count), f32),
            pltpu.VMEM((2, edge_count), jnp.int32),
            pltpu.VMEM((edge_count,), f32),
            pltpu.VMEM((3, edge_count), f32),
            pltpu.VMEM((24 * tiles, run), f32),
            pltpu.VMEM((8, edge_count), f32),
            pltpu.VMEM((8, count), f32),
            pltpu.VMEM((4 * rows, depth), f32),
            pltpu.VMEM((3 * rows, depth), f32),
            pltpu.VMEM((rows, run), f32),
            pltpu.VMEM((up(plan.cols, 8), count), f32),
        ]
        scratch += [pltpu.VMEM((rows if n in (4, 5) else 3 * h, run), f32) for n in range(8)]
        scratch += [pltpu.VMEM((3 * depth, 3 * run), bf16) for _ in range(3)]
        scratch += [
            pltpu.VMEM((19 * h, depth), f32),
            pltpu.SemaphoreType.DMA((4, 8)),
            pltpu.SemaphoreType.DMA((6,)),
            pltpu.SemaphoreType.REGULAR((8,)),
        ]
        vmem = pl.BlockSpec(memory_space=pltpu.VMEM)
        far = pl.BlockSpec(memory_space=pltpu.HBM)

        def exchange(*refs):
            exchange_kernel(plan, nx, ny, *refs)

        def finish(*refs):
            finish_kernel(plan, *refs)

        held = pl.pallas_call(
            exchange,
            out_shape=(
                jax.ShapeDtypeStruct((19 * wx * wy, depth), f32),
                jax.ShapeDtypeStruct((3 * rows, depth), f32),
                jax.ShapeDtypeStruct((rows, count), f32),
                jax.ShapeDtypeStruct((2 * depth, count), bf16),
            ),
            in_specs=[far] * 6,
            out_specs=(vmem,) * 4,
            scratch_shapes=scratch,
            compiler_params=pltpu.CompilerParams(
                collective_id=0, has_side_effects=True, vmem_limit_bytes=24 * 1024 * 1024
            ),
            name="exchange",
        )(
            *[
                pltpu.with_memory_space_constraint(value, pltpu.HBM)
                for value in (
                    populations.reshape(19 * wx * wy, depth),
                    vert_base,
                    vert_frac,
                    edges,
                    stiffness,
                    rest,
                )
            ]
        )
        fresh, sampled = pl.pallas_call(
            finish,
            out_shape=(
                jax.ShapeDtypeStruct((19 * wx * wy, depth), f32),
                jax.ShapeDtypeStruct((3, count), f32),
            ),
            in_specs=[vmem] * 4,
            out_specs=(far, far),
            scratch_shapes=[pltpu.VMEM((3, count), f32), pltpu.SemaphoreType.DMA((5,))],
            compiler_params=pltpu.CompilerParams(vmem_limit_bytes=24 * 1024 * 1024),
            name="finish",
        )(*held)
        return fresh.reshape(19, wx, wy, depth), sampled

    placed = (
        P(None, "gx", "gy", None),
        P(None, ("gx", "gy")),
        P(None, ("gx", "gy")),
        P(None, ("gx", "gy")),
        P(("gx", "gy")),
        P(None, ("gx", "gy")),
    )
    return jax.shard_map(
        per_device,
        mesh=mesh,
        in_specs=placed,
        out_specs=(P(None, "gx", "gy", None), P(None, ("gx", "gy"))),
        check_vma=False,
    )
```

```python
import jax
import jax.numpy as jnp
from jax import lax
from jax.experimental import pallas as pl
from jax.experimental.pallas import tpu as pltpu
from jax.sharding import PartitionSpec as P

lattice_speeds = [
    (0, 0, 0),
    (1, 0, 0),
    (-1, 0, 0),
    (0, 1, 0),
    (0, -1, 0),
    (0, 0, 1),
    (0, 0, -1),
    (1, 1, 0),
    (-1, -1, 0),
    (1, -1, 0),
    (-1, 1, 0),
    (1, 0, 1),
    (-1, 0, -1),
    (1, 0, -1),
    (-1, 0, 1),
    (0, 1, 1),
    (0, -1, -1),
    (0, 1, -1),
    (0, -1, 1),
]
lattice_weights = [1.0 / 3.0] + [1.0 / 18.0] * 6 + [1.0 / 36.0] * 12
relax_time = 0.9
run = 128
window = 8
sides = [(1, 1), (1, -1), (-1, 1), (-1, -1), (0, 1), (0, -1), (1, 0), (-1, 0)]
groups = [(0, 1, 6), (2, 3, 7), (4,), (5,)]
f32, bf16 = jnp.float32, jnp.bfloat16


def outer_weight(r):
    return (5.0 - 2.0 * r - jnp.sqrt(-7.0 + 12.0 * r - 4.0 * r * r)) / 8.0


def inner_weight(r):
    return (3.0 - 2.0 * r + jnp.sqrt(1.0 + 4.0 * r - 4.0 * r * r)) / 8.0


def up(n, m):
    return (n + m - 1) // m * m


class Plan:
    def __init__(self, wx, wy):
        self.wx, self.wy, self.own = wx, wy, wx * wy
        self.h = up(wy + 3, 8)
        self.cols = wx + 3
        self.rows = up(self.cols * self.h, 16)
        self.xs = list(range(-1, wx + 2))

        def span(d, w):
            return {0: list(range(-1, w + 2)), 1: [w - 1, w, w + 1], -1: [-1, 0, 1]}[d]

        def edge(d, w):
            return {0: list(range(w)), 1: [w - 1], -1: [0, 1]}[d]

        def near(d, w):
            return {0: list(range(w)), 1: [w - 1], -1: [0]}[d]

        def cells(d, pick):
            xs, ys = pick(d[0], wx), pick(d[1], wy)
            if d[0]:
                return [(x, y) for x in xs for y in ys]
            return [(x, y) for y in ys for x in xs]

        self.edge = [cells(d, edge) for d in sides]
        self.near = [cells(d, near) for d in sides]
        self.force = [cells(d, span) for d in sides]
        self.dirs = [
            [
                q
                for q, c in enumerate(lattice_speeds)
                if (not d[0] or c[0] == d[0]) and (not d[1] or c[1] == d[1])
            ]
            for d in sides
        ]
        self.macro_rows = [
            4 * len(e) + len(q) * len(n) + 1 for e, q, n in zip(self.edge, self.dirs, self.near)
        ]
        self.force_rows = [3 * self.h if d[1] == 0 else len(c) for d, c in zip(sides, self.force)]

    def row(self, x, y):
        return (x + 1) * self.h + y % self.h

    def there(self, cell, d):
        return self.row(cell[0] - d[0] * self.wx, cell[1] - d[1] * self.wy)

    def late(self, x):
        return x < 2 or x > self.wx - 2


def runs(src, dst):
    out, i = [], 0
    while i < len(src):
        n, a, b = 1, 1, 1
        if i + 1 < len(src) and src[i + 1] > src[i] and dst[i + 1] > dst[i]:
            a, b = src[i + 1] - src[i], dst[i + 1] - dst[i]
            n = 2
            while i + n < len(src) and src[i + n] - src[i + n - 1] == a and dst[i + n] - dst[i + n - 1] == b:
                n += 1
        out.append((src[i], a, dst[i], b, n))
        i += n
    return out


def ds(start, n, stride):
    return pl.ds(start, n, stride=stride) if stride > 1 else pl.ds(start, n)


def move(src_ref, src, dst_ref, dst):
    for s, a, d, b, n in runs(src, dst):
        dst_ref[ds(d, n, b), :] = src_ref[ds(s, n, a), :]


def split(value):
    high = value.astype(bf16)
    return high, (value - high.astype(f32)).astype(bf16)


def halves(value):
    return jnp.concatenate(split(value), axis=0)


def pick4(delta, weights):
    out = jnp.zeros(delta.shape, f32)
    for k in range(4):
        out = jnp.where(delta == k, weights[k], out)
    return out


def wrap(value, depth):
    value = jnp.where(value < 0, value + depth, value)
    return jnp.where(value >= depth, value - depth, value)


def along_speed(c, vector):
    total = None
    for k in range(3):
        if c[k]:
            term = vector[k] if c[k] > 0 else -vector[k]
            total = term if total is None else total + term
    return total


def transposed_dot(a, b):
    return lax.dot_general(a, b, (((1,), (1,)), ((), ())), preferred_element_type=f32)


def exchange_kernel(plan, nx, ny, *refs):
    wx, wy, h, rows, own = plan.wx, plan.wy, plan.h, plan.rows, plan.own
    sources, (fresh, sampled), scratch = refs[0:6], refs[6:8], refs[8:]
    ms, mr, fs, fr = scratch[0:8], scratch[8:16], scratch[16:24], scratch[24:32]
    (pops, base, frac, edges, stiff, rest, pos, pull, mem, mac, grid, comb, px_ref) = scratch[32:45]
    placed = scratch[45:53]
    ones_y, ones_l, ones_r, edge_pops, vel, plane, along, part_sum, sems, load_sems, ready = scratch[53:]
    depth = pops.shape[1]
    load_into = (pops.at[pl.ds(0, 19 * own), :], base, frac, edges, stiff, rest)
    loads_in = [pltpu.make_async_copy(sources[n], load_into[n], load_sems.at[n]) for n in range(6)]
    for n in (3, 2, 1, 5, 4, 0):
        loads_in[n].start()
    count = base.shape[1]
    edge_count = edges.shape[1]
    tiles = count // run
    ix, iy = lax.axis_index("gx"), lax.axis_index("gy")
    peers = [(lax.rem(ix + dx + nx, nx), lax.rem(iy + dy + ny, ny)) for dx, dy in sides]

    def rank(px, py):
        return px * ny + py

    key = rank(ix, iy)
    lead = [(key < rank(px, py)).astype(jnp.int32) for px, py in peers]
    led = [sum(lead[n] for n in g) for g in groups]
    barrier = pltpu.get_barrier_semaphore()

    def hail(sem, n):
        pl.semaphore_signal(sem, inc=1, device_id=peers[n], device_id_type=pl.DeviceIdType.MESH)

    for n in range(8):

        @pl.when(lead[n] == 1)
        def _():
            hail(barrier, n)

    def copies(src, dst, kind):
        return [
            pltpu.make_async_remote_copy(
                src_ref=src[n],
                dst_ref=dst[n],
                send_sem=sems.at[0],
                recv_sem=sems.at[kind + (0 if n in (4, 5) else 1)],
                device_id=peers[n],
                device_id_type=pl.DeviceIdType.MESH,
            )
            for n in range(8)
        ]

    first_col = {1: wx, -1: 0}
    outgoing = list(fs)
    for n in (6, 7):
        outgoing[n] = comb.at[pl.ds(first_col[sides[n][0]] * h, 3 * h), :]
    macro_copies = copies(ms, mr, 1)
    force_copies = copies(outgoing, fr, 3)

    def arrive(kind, which):
        lengths = plan.macro_rows if kind == 1 else plan.force_rows
        all_of = pops.at[pl.ds(0, sum(lengths[n] for n in which)), :]
        pltpu.make_async_remote_copy(
            src_ref=all_of,
            dst_ref=all_of,
            send_sem=sems.at[0],
            recv_sem=sems.at[kind + (0 if 4 in which else 1)],
            device_id=peers[0],
            device_id_type=pl.DeviceIdType.MESH,
        ).wait_recv()

    zeros = jnp.zeros((8, run), f32)
    pos[...] = jnp.zeros(pos.shape, f32)
    pull[...] = jnp.zeros(pull.shape, f32)
    for ref in placed:
        ref[...] = jnp.zeros(ref.shape, f32)
    for n in (3, 2, 1, 5, 4):
        loads_in[n].wait()

    moved = frac[...]
    weights = [
        outer_weight(1.0 + moved),
        inner_weight(moved),
        inner_weight(1.0 - moved),
        outer_weight(2.0 - moved),
    ]
    lane = lax.broadcasted_iota(jnp.int32, (1, run), 1)
    slot = lax.rem(lane, window)
    of_tile = lax.rem(lane // window, tiles)
    start_of = jnp.zeros((1, run), jnp.int32)
    offsets = []
    for t in range(tiles):
        z = base[2:3, t * run : (t + 1) * run]
        gap = z - z[0:1, 0:1]
        gap = jnp.where(gap > depth // 2, gap - depth, gap)
        gap = jnp.where(gap < -(depth // 2), gap + depth, gap)
        low = jnp.min(gap, axis=1, keepdims=True)
        offsets.append(gap - low)
        start_of = jnp.where(of_tile == t, z[0:1, 0:1] + low - 1, start_of)
    zmap = wrap(start_of + slot, depth).astype(f32)
    offset = jnp.concatenate(offsets, axis=1)
    reach_z = pick4(lax.broadcasted_iota(jnp.int32, (window, count), 0) - offset, [w[2:3] for w in weights])

    part = 8 * tiles
    high = moved.astype(bf16).astype(f32)
    low = moved - high
    whole = base[...].astype(f32)
    for t in range(tiles):
        cols = slice(t * run, (t + 1) * run)
        pos[pl.ds(8 * t, 3), :] = whole[:, cols]
        pos[pl.ds(part + 8 * t, 3), :] = high[:, cols]
        pos[pl.ds(2 * part + 8 * t, 3), :] = low[:, cols]
    ends = edges[...]
    spot = lax.broadcasted_iota(jnp.int32, (run, edge_count), 0)
    tail = jnp.bitwise_and(ends[0:1], run - 1)
    head = jnp.bitwise_and(ends[1:2], run - 1)
    hot = jnp.where(spot == head, 1.0, jnp.where(spot == tail, -1.0, 0.0)).astype(bf16)
    group = lax.shift_right_logical(ends[0:1], run.bit_length() - 1)
    reach = jnp.dot(pos[...].astype(bf16), hot, preferred_element_type=f32)
    reach = reach[0:part] + reach[part : 2 * part] + reach[2 * part : 3 * part]
    def moments(r):
        totals = [None] * 4
        for q, c in enumerate(lattice_speeds):
            value = pops[pl.ds(q * own + r, 8), :]
            for k, sign in enumerate((1,) + c):
                if sign:
                    term = value if sign > 0 else -value
                    totals[k] = term if totals[k] is None else totals[k] + term
        for k in range(4):
            for i in range(0, 8, wy):
                mac[pl.ds(k * rows + plan.row((r + i) // wy, 0), wy), :] = totals[k][i : i + wy]

    def pack(n):
        cells, close = plan.edge[n], plan.near[n]
        for k in range(4):
            move(
                mac,
                [k * rows + plan.row(x, y) for x, y in cells],
                ms[n],
                [k * len(cells) + i for i in range(len(cells))],
            )
        for s, q in enumerate(plan.dirs[n]):
            first = 4 * len(cells) + s * len(close)
            move(pops, [q * own + x * wy + y for x, y in close], ms[n], [first + i for i in range(len(close))])
        ms[n][pl.ds(plan.macro_rows[n] - 1, 1), :] = zmap

    late = (0, 1, 6, 2, 3, 7)
    ends_of = sorted({x * wy // 8 * 8 for x in (0, 1, wx - 1)})
    loads_in[0].wait()
    for r in ends_of:
        moments(r)
    for n in late:
        pack(n)
    pull[pl.ds(0, 3), :] = rest[...]
    diff = jnp.zeros((8, edge_count), f32)
    for t in range(tiles):
        diff = jnp.where(group == t, reach[8 * t : 8 * t + 8], diff)
    stretch = stiff[...].reshape(1, edge_count) * (diff - pull[...])
    terms = jnp.concatenate([jnp.where(group == t, stretch, 0.0) for t in range(tiles)], axis=0)
    summed = transposed_dot(halves(terms), hot)
    summed = summed[0:part] + summed[part : 2 * part]
    for t in range(tiles):
        mem[:, t * run : (t + 1) * run] = -summed[8 * t : 8 * t + 8]

    bx = base[0:1, :] - ix * wx - 1
    by = base[1:2, :] - iy * wy - 1
    i = lax.broadcasted_iota(jnp.int32, (px_ref.shape[0], 1), 0)
    px_ref[...] = pick4(i - 1 - bx, [w[0:1] for w in weights])
    i = lax.broadcasted_iota(jnp.int32, (h, 1), 0)
    y = jnp.where(i == h - 1, -1, jnp.where(i > wy + 1, -100, i))
    py = pick4(y - by, [w[1:2] for w in weights])
    for k in range(rows // h):
        if k < plan.cols:
            plane[pl.ds(k * h, h), :] = px_ref[pl.ds(k, 1), :] * py
        else:
            plane[pl.ds(k * h, h), :] = jnp.zeros((h, count), f32)

    big, small = [], []
    for c in range(3):
        for t in range(tiles):
            cols = slice(t * run, (t + 1) * run)
            block = reach_z[:, cols] * mem[c : c + 1, cols]
            rounded = block.astype(bf16).astype(f32)
            for out, value in ((big, rounded), (small, block - rounded)):
                out.append(jnp.concatenate([value if t == s else zeros for s in range(tiles)], axis=1))
    pad = [jnp.zeros((run - 3 * tiles * window, count), f32)]
    spread = transposed_dot(halves(plane[...]), jnp.concatenate(big + pad + small + pad, axis=0).astype(bf16))
    spread = spread[0:rows] + spread[rows : 2 * rows]
    comb[...] = spread[:, 0:run] + spread[:, run : 2 * run]
    for n in range(6):
        move(comb, [plan.row(x, y) for x, y in plan.force[n]], fs[n], list(range(plan.force_rows[n])))
    greetings = 8 - sum(lead)

    @pl.when(greetings > 0)
    def _():
        pl.semaphore_wait(barrier, greetings)

    for n in range(8):
        back = sides.index((-sides[n][0], -sides[n][1]))
        slot_of = [i for i, g in enumerate(groups) if back in g][0]

        @pl.when(lead[n] == 0)
        def _():
            hail(ready.at[slot_of], n)

    for n in late:

        @pl.when(lead[n] == 0)
        def _():
            force_copies[n].start()
            macro_copies[n].start()

    for n in (4, 5):

        @pl.when(lead[n] == 0)
        def _():
            force_copies[n].start()

    for r in range(0, own, 8):
        if r not in ends_of:
            moments(r)
    for n in (4, 5):
        pack(n)

    for n in (4, 5):

        @pl.when(lead[n] == 0)
        def _():
            macro_copies[n].start()

    for i in (2, 3, 0, 1):

        @pl.when(led[i] > 0)
        def _():
            pl.semaphore_wait(ready.at[i], led[i])

        for n in groups[i]:

            @pl.when(lead[n] == 1)
            def _():
                force_copies[n].start()
                macro_copies[n].start()

    gap = wrap(lax.broadcasted_iota(jnp.int32, (depth, count), 0) - (base[2:3, :] - 1), depth)
    z_high, z_low = split(pick4(gap, [w[2:3] for w in weights]))
    along[pl.ds(0, depth), :] = z_high
    along[pl.ds(depth, depth), :] = z_low

    comp_of = lane // (window * tiles)
    comps_of = jnp.concatenate([comp_of] * 3, axis=1)

    def mark(ones, s, zrow):
        at = jnp.where(lax.broadcasted_iota(jnp.int32, (depth, run), 0).astype(f32) == zrow, 1.0, 0.0)
        if ones.shape[0] == depth:
            ones[:, pl.ds(s * run, run)] = at.astype(bf16)
            return
        for c in range(3):
            ones[pl.ds(c * depth, depth), pl.ds(s * run, run)] = jnp.where(comp_of == c, at, 0.0).astype(bf16)

    def take_macro(n):
        cells, close, d = plan.edge[n], plan.near[n], sides[n]
        for k in range(4):
            move(
                mr[n],
                [k * len(cells) + i for i in range(len(cells))],
                mac,
                [k * rows + plan.there(c, d) for c in cells],
            )
        return mr[n][pl.ds(plan.macro_rows[n] - 1, 1), :]

    def pop_row(n, q, cell):
        cells, close = plan.edge[n], plan.near[n]
        return 4 * len(cells) + plan.dirs[n].index(q) * len(close) + close.index(cell)

    keep = 1.0 - 1.0 / relax_time
    half = 1.0 - 0.5 / relax_time
    level_row = lax.broadcasted_iota(jnp.int32, (h, 1), 0)

    def population(q, x):
        c = lattice_speeds[q]
        if x < 0 or x >= wx:
            return edge_pops[pl.ds(q * h, h), :]
        value = pops[pl.ds(q * own + x * wy, h), :]
        if c[1] == 1:
            value = jnp.where(level_row == h - 1, mr[4][pl.ds(pop_row(4, q, (x, wy - 1)), 1), :], value)
        if c[1] == -1:
            value = jnp.where(level_row == wy, mr[5][pl.ds(pop_row(5, q, (x, 0)), 1), :], value)
        return value

    def collide(x):
        at = (x + 1) * h
        density = mac[pl.ds(at, h), :]
        force = [grid[pl.ds(k * rows + at, h), :] for k in range(3)]
        inverse = 1.0 / density
        speed = [(mac[pl.ds((k + 1) * rows + at, h), :] + 0.5 * force[k]) * inverse for k in range(3)]
        for k in range(3):
            held = jnp.where((level_row <= wy + 1) | (level_row == h - 1), speed[k], 0.0)
            vel[pl.ds(k * rows + at, h), :] = held
        square = speed[0] * speed[0] + speed[1] * speed[1] + speed[2] * speed[2]
        work = speed[0] * force[0] + speed[1] * force[1] + speed[2] * force[2]
        scaled = density * (1.0 / relax_time)
        level = scaled * (1.0 - 1.5 * square) - (3.0 * half) * work
        for first in [0] + list(range(1, 19, 2)):
            pair = [0] if first == 0 else [first, first + 1]
            pair = [q for q in pair if 0 <= x + lattice_speeds[q][0] < wx]
            if not pair:
                continue
            weight = lattice_weights[first]
            if first == 0:
                even, odd = level * weight, None
            else:
                a = along_speed(lattice_speeds[first], speed)
                push = along_speed(lattice_speeds[first], force)
                turn = scaled * a + half * push
                even = weight * (level + a * (4.5 * scaled * a + 9.0 * half * push))
                odd = (3.0 * weight) * turn
            for q in pair:
                c = lattice_speeds[q]
                value = keep * population(q, x) + even
                if odd is not None:
                    value = value + odd if q == first else value - odd
                if c[1]:
                    value = pltpu.roll(value, c[1] % h, 0)
                if c[2]:
                    value = pltpu.roll(value, c[2] % depth, 1)
                fresh[pl.ds(q * own + (x + c[0]) * wy, wy), :] = value[0:wy]

    mark(ones_y, 0, zmap)
    arrive(1, (4, 5))
    for s, n in ((1, 4), (2, 5)):
        mark(ones_y, s, take_macro(n))
    arrive(3, (4, 5))
    for n in (4, 5):
        move(fr[n], list(range(plan.force_rows[n])), placed[n], [plan.there(c, sides[n]) for c in plan.force[n]])

    def widen(parts, ones):
        value = transposed_dot(halves(jnp.concatenate(parts, axis=1)), ones[...])
        half_rows = value.shape[0] // 2
        return value[0:half_rows] + value[half_rows:]

    value = widen([comb[...], placed[4][...], placed[5][...]], ones_y)
    for c in range(3):
        grid[pl.ds(c * rows, rows), :] = value[:, c * depth : (c + 1) * depth]
    for x in plan.xs:
        if not plan.late(x):
            collide(x)

    def sample(spans):
        flat = jnp.concatenate([plane[pl.ds(a, n), :] for a, n in spans], axis=0)
        value = jnp.concatenate([vel[pl.ds(k * rows + a, n), :] for k in range(3) for a, n in spans], axis=0)
        v_high, v_low = split(value)
        value = jnp.dot(
            jnp.concatenate(
                [
                    jnp.concatenate([v_high, v_high], axis=1),
                    jnp.concatenate([v_low, jnp.zeros(v_low.shape, bf16)], axis=1),
                ],
                axis=0,
            ),
            along[...],
            preferred_element_type=f32,
        )
        size = flat.shape[0]
        out = []
        for k in range(3):
            both = value[k * size : (k + 1) * size] + value[(k + 3) * size : (k + 4) * size]
            both = both * flat
            acc = both[0:8]
            for r in range(8, size, 8):
                acc = acc + both[r : r + 8]
            out.append(acc)
        return out

    left, right = 3 * h, wx * h
    for k, value in enumerate(sample([(left, right - left)])):
        part_sum[pl.ds(8 * k, 8), :] = value

    arrive(1, late)
    for ones, order in ((ones_l, (6, 0, 1)), (ones_r, (7, 2, 3))):
        for s, n in enumerate(order):
            mark(ones, s, take_macro(n))
            for q in plan.dirs[n]:
                close = plan.near[n]
                src = [pop_row(n, q, c) for c in close]
                move(mr[n], src, edge_pops, [q * h + (c[1] - sides[n][1] * wy) % h for c in close])
    arrive(3, late)
    for ones, order, at in ((ones_l, (6, 0, 1), 0), (ones_r, (7, 2, 3), right)):
        for n in order[1:]:
            dst = [plan.there(c, sides[n]) - at for c in plan.force[n]]
            move(fr[n], list(range(plan.force_rows[n])), placed[n], dst)
        parts = jnp.concatenate([fr[order[0]][...], placed[order[1]][...], placed[order[2]][...]], axis=1)
        parts = jnp.concatenate([jnp.where(comps_of == c, parts, 0.0) for c in range(3)], axis=0)
        value = transposed_dot(halves(parts), ones[...])
        for c in range(3):
            here = pl.ds(c * rows + at, 3 * h)
            both = value[3 * h * c : 3 * h * (c + 1)] + value[3 * h * (c + 3) : 3 * h * (c + 4)]
            grid[here, :] = grid[here, :] + both
    for x in plan.xs:
        if plan.late(x):
            collide(x)
    for k, value in enumerate(sample([(0, left), (right, 3 * h)])):
        value = value + part_sum[pl.ds(8 * k, 8), :]
        sampled[k : k + 1, :] = jnp.sum(value, axis=0, keepdims=True)
    sent = pops.at[pl.ds(0, sum(plan.macro_rows) + sum(plan.force_rows)), :]
    pltpu.make_async_remote_copy(
        src_ref=sent,
        dst_ref=sent,
        send_sem=sems.at[0],
        recv_sem=sems.at[1],
        device_id=peers[0],
        device_id_type=pl.DeviceIdType.MESH,
    ).wait_send()


def finish_kernel(fresh, sampled, fresh_out, sampled_out, sems):
    leave = [pltpu.make_async_copy(fresh, fresh_out, sems.at[0]), pltpu.make_async_copy(sampled, sampled_out, sems.at[1])]
    for copy in leave:
        copy.start()
    for copy in leave:
        copy.wait()


def solution(mesh):
    nx, ny = mesh.shape["gx"], mesh.shape["gy"]

    def per_device(populations, vert_base, vert_frac, edges, stiffness, rest):
        _, wx, wy, depth = populations.shape
        count, edge_count = vert_base.shape[1], edges.shape[1]
        plan = Plan(wx, wy)
        rows, tiles, h = plan.rows, count // run, plan.h
        macro = [pltpu.VMEM((n, depth), f32) for n in plan.macro_rows]
        force = [pltpu.VMEM((n, run), f32) for n in plan.force_rows]
        scratch = macro + macro + force + force
        scratch += [
            pltpu.VMEM((19 * wx * wy + h, depth), f32),
            pltpu.VMEM((3, count), jnp.int32),
            pltpu.VMEM((3, count), f32),
            pltpu.VMEM((2, edge_count), jnp.int32),
            pltpu.VMEM((edge_count,), f32),
            pltpu.VMEM((3, edge_count), f32),
            pltpu.VMEM((24 * tiles, run), f32),
            pltpu.VMEM((8, edge_count), f32),
            pltpu.VMEM((8, count), f32),
            pltpu.VMEM((4 * rows, depth), f32),
            pltpu.VMEM((3 * rows, depth), f32),
            pltpu.VMEM((rows, run), f32),
            pltpu.VMEM((up(plan.cols, 8), count), f32),
        ]
        scratch += [pltpu.VMEM((rows if n in (4, 5) else 3 * h, run), f32) for n in range(8)]
        scratch += [pltpu.VMEM((n * depth, 3 * run), bf16) for n in (3, 1, 1)]
        scratch += [
            pltpu.VMEM((19 * h, depth), f32),
            pltpu.VMEM((3 * rows, depth), f32),
            pltpu.VMEM((rows, count), f32),
            pltpu.VMEM((2 * depth, count), bf16),
            pltpu.VMEM((24, count), f32),
            pltpu.SemaphoreType.DMA((5,)),
            pltpu.SemaphoreType.DMA((6,)),
            pltpu.SemaphoreType.REGULAR((len(groups),)),
        ]
        vmem = pl.BlockSpec(memory_space=pltpu.VMEM)
        far = pl.BlockSpec(memory_space=pltpu.HBM)

        def exchange(*refs):
            exchange_kernel(plan, nx, ny, *refs)

        held = pl.pallas_call(
            exchange,
            out_shape=(
                jax.ShapeDtypeStruct((19 * wx * wy, depth), f32),
                jax.ShapeDtypeStruct((3, count), f32),
            ),
            in_specs=[far] * 6,
            out_specs=(vmem,) * 2,
            scratch_shapes=scratch,
            compiler_params=pltpu.CompilerParams(
                collective_id=0, has_side_effects=True, vmem_limit_bytes=24 * 1024 * 1024
            ),
            name="exchange",
        )(
            *[
                pltpu.with_memory_space_constraint(value, pltpu.HBM)
                for value in (
                    populations.reshape(19 * wx * wy, depth),
                    vert_base,
                    vert_frac,
                    edges,
                    stiffness,
                    rest,
                )
            ]
        )
        fresh, sampled = pl.pallas_call(
            finish_kernel,
            out_shape=(
                jax.ShapeDtypeStruct((19 * wx * wy, depth), f32),
                jax.ShapeDtypeStruct((3, count), f32),
            ),
            in_specs=[vmem] * 2,
            out_specs=(far, far),
            scratch_shapes=[pltpu.SemaphoreType.DMA((2,))],
            compiler_params=pltpu.CompilerParams(vmem_limit_bytes=24 * 1024 * 1024),
            name="finish",
        )(*held)
        return fresh.reshape(19, wx, wy, depth), sampled

    placed = (
        P(None, "gx", "gy", None),
        P(None, ("gx", "gy")),
        P(None, ("gx", "gy")),
        P(None, ("gx", "gy")),
        P(("gx", "gy")),
        P(None, ("gx", "gy")),
    )
    return jax.shard_map(
        per_device,
        mesh=mesh,
        in_specs=placed,
        out_specs=(P(None, "gx", "gy", None), P(None, ("gx", "gy"))),
        check_vma=False,
    )
```

```python
import jax
import jax.numpy as jnp
from jax import lax
from jax.experimental import pallas as pl
from jax.experimental.pallas import tpu as pltpu
from jax.sharding import PartitionSpec as P

lattice_speeds = [
    (0, 0, 0),
    (1, 0, 0),
    (-1, 0, 0),
    (0, 1, 0),
    (0, -1, 0),
    (0, 0, 1),
    (0, 0, -1),
    (1, 1, 0),
    (-1, -1, 0),
    (1, -1, 0),
    (-1, 1, 0),
    (1, 0, 1),
    (-1, 0, -1),
    (1, 0, -1),
    (-1, 0, 1),
    (0, 1, 1),
    (0, -1, -1),
    (0, 1, -1),
    (0, -1, 1),
]
lattice_weights = [1.0 / 3.0] + [1.0 / 18.0] * 6 + [1.0 / 36.0] * 12
relax_time = 0.9
run = 128
window = 8
pieces = 1
sides = [(1, 1), (1, -1), (-1, 1), (-1, -1), (0, 1), (0, -1), (1, 0), (-1, 0)]
groups = [(0, 1, 6), (2, 3, 7), (4,), (5,)]
f32, bf16 = jnp.float32, jnp.bfloat16


def outer_weight(r):
    return (5.0 - 2.0 * r - jnp.sqrt(-7.0 + 12.0 * r - 4.0 * r * r)) / 8.0


def inner_weight(r):
    return (3.0 - 2.0 * r + jnp.sqrt(1.0 + 4.0 * r - 4.0 * r * r)) / 8.0


def up(n, m):
    return (n + m - 1) // m * m


class Plan:
    def __init__(self, wx, wy):
        self.wx, self.wy, self.own = wx, wy, wx * wy
        self.h = up(wy + 3, 8)
        self.cols = wx + 3
        self.rows = up(self.cols * self.h, 16)
        self.xs = list(range(-1, wx + 2))

        def span(d, w):
            return {0: list(range(-1, w + 2)), 1: [w - 1, w, w + 1], -1: [-1, 0, 1]}[d]

        def edge(d, w):
            return {0: list(range(w)), 1: [w - 1], -1: [0, 1]}[d]

        def near(d, w):
            return {0: list(range(w)), 1: [w - 1], -1: [0]}[d]

        def cells(d, pick):
            xs, ys = pick(d[0], wx), pick(d[1], wy)
            if d[0]:
                return [(x, y) for x in xs for y in ys]
            return [(x, y) for y in ys for x in xs]

        self.edge = [cells(d, edge) for d in sides]
        self.near = [cells(d, near) for d in sides]
        self.force = [cells(d, span) for d in sides]
        self.dirs = [
            [
                q
                for q, c in enumerate(lattice_speeds)
                if (not d[0] or c[0] == d[0]) and (not d[1] or c[1] == d[1])
            ]
            for d in sides
        ]
        self.macro_rows = [
            4 * len(e) + len(q) * len(n) + 1 for e, q, n in zip(self.edge, self.dirs, self.near)
        ]
        self.force_rows = [3 * self.h if d[1] == 0 else len(c) for d, c in zip(sides, self.force)]

    def row(self, x, y):
        return (x + 1) * self.h + y % self.h

    def there(self, cell, d):
        return self.row(cell[0] - d[0] * self.wx, cell[1] - d[1] * self.wy)

    def late(self, x):
        return x < 2 or x > self.wx - 2


def runs(src, dst):
    out, i = [], 0
    while i < len(src):
        n, a, b = 1, 1, 1
        if i + 1 < len(src) and src[i + 1] > src[i] and dst[i + 1] > dst[i]:
            a, b = src[i + 1] - src[i], dst[i + 1] - dst[i]
            n = 2
            while i + n < len(src) and src[i + n] - src[i + n - 1] == a and dst[i + n] - dst[i + n - 1] == b:
                n += 1
        out.append((src[i], a, dst[i], b, n))
        i += n
    return out


def ds(start, n, stride):
    return pl.ds(start, n, stride=stride) if stride > 1 else pl.ds(start, n)


def move(src_ref, src, dst_ref, dst):
    for s, a, d, b, n in runs(src, dst):
        dst_ref[ds(d, n, b), :] = src_ref[ds(s, n, a), :]


def split(value):
    high = value.astype(bf16)
    return high, (value - high.astype(f32)).astype(bf16)


def halves(value):
    return jnp.concatenate(split(value), axis=0)


def pick4(delta, weights):
    out = jnp.zeros(delta.shape, f32)
    for k in range(4):
        out = jnp.where(delta == k, weights[k], out)
    return out


def wrap(value, depth):
    value = jnp.where(value < 0, value + depth, value)
    return jnp.where(value >= depth, value - depth, value)


def along_speed(c, vector):
    total = None
    for k in range(3):
        if c[k]:
            term = vector[k] if c[k] > 0 else -vector[k]
            total = term if total is None else total + term
    return total


def transposed_dot(a, b):
    return lax.dot_general(a, b, (((1,), (1,)), ((), ())), preferred_element_type=f32)


def sample(vel, plane, along, rows, spans):
    flat = jnp.concatenate([plane[pl.ds(a, n), :] for a, n in spans], axis=0)
    value = jnp.concatenate([vel[pl.ds(k * rows + a, n), :] for k in range(3) for a, n in spans], axis=0)
    v_high, v_low = split(value)
    value = jnp.dot(
        jnp.concatenate(
            [
                jnp.concatenate([v_high, v_high], axis=1),
                jnp.concatenate([v_low, jnp.zeros(v_low.shape, bf16)], axis=1),
            ],
            axis=0,
        ),
        along[...],
        preferred_element_type=f32,
    )
    size = flat.shape[0]
    out = []
    for k in range(3):
        both = value[k * size : (k + 1) * size] + value[(k + 3) * size : (k + 4) * size]
        both = both * flat
        acc = both[0:8]
        for r in range(8, size, 8):
            acc = acc + both[r : r + 8]
        out.append(acc)
    return out


def exchange_kernel(plan, nx, ny, *refs):
    wx, wy, h, rows, own = plan.wx, plan.wy, plan.h, plan.rows, plan.own
    sources, scratch = refs[0:6], refs[11:]
    fresh, vel, plane, along, part_sum = refs[6:11]
    ms, mr, fs, fr = scratch[0:8], scratch[8:16], scratch[16:24], scratch[24:32]
    (pops, base, frac, edges, stiff, rest, pos, pull, mem, mac, grid, comb, px_ref) = scratch[32:45]
    placed = scratch[45:53]
    ones_y, ones_l, ones_r, edge_pops, sems, load_sems, ready = scratch[53:]
    depth = pops.shape[1]
    load_into = (pops.at[pl.ds(0, 19 * own), :], base, frac, edges, stiff, rest)
    loads_in = [pltpu.make_async_copy(sources[n], load_into[n], load_sems.at[n]) for n in range(6)]
    for n in (3, 2, 1, 5, 4, 0):
        loads_in[n].start()
    count = base.shape[1]
    edge_count = edges.shape[1]
    tiles = count // run
    ix, iy = lax.axis_index("gx"), lax.axis_index("gy")
    peers = [(lax.rem(ix + dx + nx, nx), lax.rem(iy + dy + ny, ny)) for dx, dy in sides]

    def rank(px, py):
        return px * ny + py

    key = rank(ix, iy)
    lead = [(key < rank(px, py)).astype(jnp.int32) for px, py in peers]
    led = [sum(lead[n] for n in g) for g in groups]
    barrier = pltpu.get_barrier_semaphore()

    def hail(sem, n):
        pl.semaphore_signal(sem, inc=1, device_id=peers[n], device_id_type=pl.DeviceIdType.MESH)

    for n in range(8):

        @pl.when(lead[n] == 1)
        def _():
            hail(barrier, n)

    def copies(src, dst, kind):
        return [
            pltpu.make_async_remote_copy(
                src_ref=src[n],
                dst_ref=dst[n],
                send_sem=sems.at[0],
                recv_sem=sems.at[kind + (0 if n in (4, 5) else 1)],
                device_id=peers[n],
                device_id_type=pl.DeviceIdType.MESH,
            )
            for n in range(8)
        ]

    first_col = {1: wx, -1: 0}
    outgoing = list(fs)
    for n in (6, 7):
        outgoing[n] = comb.at[pl.ds(first_col[sides[n][0]] * h, 3 * h), :]
    macro_copies = copies(ms, mr, 1)
    force_copies = copies(outgoing, fr, 3)

    def arrive(kind, which):
        lengths = plan.macro_rows if kind == 1 else plan.force_rows
        all_of = pops.at[pl.ds(0, sum(lengths[n] for n in which)), :]
        pltpu.make_async_remote_copy(
            src_ref=all_of,
            dst_ref=all_of,
            send_sem=sems.at[0],
            recv_sem=sems.at[kind + (0 if 4 in which else 1)],
            device_id=peers[0],
            device_id_type=pl.DeviceIdType.MESH,
        ).wait_recv()

    zeros = jnp.zeros((8, run), f32)
    comb[...] = jnp.zeros(comb.shape, f32)
    pos[...] = jnp.zeros(pos.shape, f32)
    pull[...] = jnp.zeros(pull.shape, f32)
    for ref in placed:
        ref[...] = jnp.zeros(ref.shape, f32)
    for n in (3, 2, 1, 5, 4):
        loads_in[n].wait()

    moved = frac[...]
    weights = [
        outer_weight(1.0 + moved),
        inner_weight(moved),
        inner_weight(1.0 - moved),
        outer_weight(2.0 - moved),
    ]
    lane = lax.broadcasted_iota(jnp.int32, (1, run), 1)
    slot = lax.rem(lane, window)
    of_tile = lax.rem(lane // window, tiles)
    start_of = jnp.zeros((1, run), jnp.int32)
    offsets = []
    for t in range(tiles):
        z = base[2:3, t * run : (t + 1) * run]
        gap = z - z[0:1, 0:1]
        gap = jnp.where(gap > depth // 2, gap - depth, gap)
        gap = jnp.where(gap < -(depth // 2), gap + depth, gap)
        low = jnp.min(gap, axis=1, keepdims=True)
        offsets.append(gap - low)
        start_of = jnp.where(of_tile == t, z[0:1, 0:1] + low - 1, start_of)
    zmap = wrap(start_of + slot, depth).astype(f32)
    offset = jnp.concatenate(offsets, axis=1)
    reach_z = pick4(lax.broadcasted_iota(jnp.int32, (window, count), 0) - offset, [w[2:3] for w in weights])

    pairs = up(tiles, 2) // 2
    ends = edges[...]
    tail = jnp.bitwise_and(ends[0:1], run - 1)
    head = jnp.bitwise_and(ends[1:2], run - 1)
    group = lax.shift_right_logical(ends[0:1], run.bit_length() - 1)
    whole = base[...].astype(f32) + moved
    for t in range(tiles):
        pos[pl.ds(4 * t, 3), :] = whole[:, t * run : (t + 1) * run]
    for k in (0, 4):
        pull[pl.ds(k, 3), :] = rest[...]
    half_of = lax.broadcasted_iota(jnp.int32, (8, edge_count), 0) // 4
    mine = [group == 2 * p + half_of for p in range(pairs)]
    diff = jnp.zeros((8, edge_count), f32)
    for p in range(pairs):
        table = pos[pl.ds(8 * p, 8), :]
        gathered = []
        for k in range(0, edge_count, run):
            at = [jnp.broadcast_to(value[:, k : k + run], (8, run)) for value in (head, tail)]
            gathered.append(
                jnp.take_along_axis(table, at[0], axis=1) - jnp.take_along_axis(table, at[1], axis=1)
            )
        diff = jnp.where(mine[p], jnp.concatenate(gathered, axis=1), diff)
    stretch = stiff[...].reshape(1, edge_count) * (diff - pull[...])
    terms = jnp.concatenate([jnp.where(mine[p], stretch, 0.0) for p in range(pairs)], axis=0)
    spot = lax.broadcasted_iota(jnp.int32, (run, edge_count), 0)
    hot = jnp.where(spot == head, 1.0, jnp.where(spot == tail, -1.0, 0.0)).astype(bf16)
    part = 8 * pairs
    summed = transposed_dot(halves(terms), hot)
    mem[...] = -(summed[0:part] + summed[part : 2 * part])

    def moments(r):
        totals = [None] * 4
        for q, c in enumerate(lattice_speeds):
            value = pops[pl.ds(q * own + r, 8), :]
            for k, sign in enumerate((1,) + c):
                if sign:
                    term = value if sign > 0 else -value
                    totals[k] = term if totals[k] is None else totals[k] + term
        for k in range(4):
            for i in range(0, 8, wy):
                mac[pl.ds(k * rows + plan.row((r + i) // wy, 0), wy), :] = totals[k][i : i + wy]

    def pack(n):
        cells, close = plan.edge[n], plan.near[n]
        for k in range(4):
            move(
                mac,
                [k * rows + plan.row(x, y) for x, y in cells],
                ms[n],
                [k * len(cells) + i for i in range(len(cells))],
            )
        for s, q in enumerate(plan.dirs[n]):
            first = 4 * len(cells) + s * len(close)
            move(pops, [q * own + x * wy + y for x, y in close], ms[n], [first + i for i in range(len(close))])
        ms[n][pl.ds(plan.macro_rows[n] - 1, 1), :] = zmap

    late = (0, 1, 6, 2, 3, 7)

    bx = base[0:1, :] - ix * wx - 1
    by = base[1:2, :] - iy * wy - 1
    i = lax.broadcasted_iota(jnp.int32, (px_ref.shape[0], 1), 0)
    px_ref[...] = pick4(i - 1 - bx, [w[0:1] for w in weights])
    i = lax.broadcasted_iota(jnp.int32, (h, 1), 0)
    y = jnp.where(i == h - 1, -1, jnp.where(i > wy + 1, -100, i))
    py = pick4(y - by, [w[1:2] for w in weights])
    big, small = [], []
    for c in range(3):
        for t in range(tiles):
            cols = slice(t * run, (t + 1) * run)
            block = reach_z[:, cols] * mem[pl.ds(4 * t + c, 1), :]
            rounded = block.astype(bf16).astype(f32)
            for out, value in ((big, rounded), (small, block - rounded)):
                out.append(jnp.concatenate([value if t == s else zeros for s in range(tiles)], axis=1))
    pad = [jnp.zeros((run - 3 * tiles * window, count), f32)]
    source = jnp.concatenate(big + pad + small + pad, axis=0).astype(bf16)

    def spread(spans):
        for a, n in spans:
            for k in range(a // h, (a + n) // h):
                plane[pl.ds(k * h, h), :] = px_ref[pl.ds(k, 1), :] * py
        flat = jnp.concatenate([plane[pl.ds(a, n), :] for a, n in spans], axis=0)
        size = flat.shape[0]
        value = transposed_dot(halves(flat), source)
        value = value[0:size] + value[size : 2 * size]
        value = value[:, 0:run] + value[:, run : 2 * run]
        done = 0
        for a, n in spans:
            comb[pl.ds(a, n), :] = value[done : done + n]
            done += n

    left, right = 3 * h, wx * h
    spread([(0, left), (right, 3 * h)])
    for n in range(4):
        move(comb, [plan.row(x, y) for x, y in plan.force[n]], fs[n], list(range(plan.force_rows[n])))
    loads_in[0].wait()
    ends_of = sorted({x * wy // 8 * 8 for x in (0, 1, wx - 1)})
    for r in ends_of:
        moments(r)
    for n in late:
        pack(n)

    greetings = 8 - sum(lead)

    @pl.when(greetings > 0)
    def _():
        pl.semaphore_wait(barrier, greetings)

    for n in range(8):
        back = sides.index((-sides[n][0], -sides[n][1]))
        slot_of = [i for i, g in enumerate(groups) if back in g][0]

        @pl.when(lead[n] == 0)
        def _():
            hail(ready.at[slot_of], n)

    for n in late:

        @pl.when(lead[n] == 0)
        def _():
            macro_copies[n].start()
            force_copies[n].start()

    for r in range(0, own, 8):
        if r not in ends_of:
            moments(r)
    for n in (4, 5):
        pack(n)

    for n in (4, 5):

        @pl.when(lead[n] == 0)
        def _():
            macro_copies[n].start()

    spread([(left, right - left)])
    for n in (4, 5):
        move(comb, [plan.row(x, y) for x, y in plan.force[n]], fs[n], list(range(plan.force_rows[n])))
    for n in (4, 5):

        @pl.when(lead[n] == 0)
        def _():
            force_copies[n].start()

    for i in (2, 3, 0, 1):

        @pl.when(led[i] > 0)
        def _():
            pl.semaphore_wait(ready.at[i], led[i])

        for n in groups[i]:

            @pl.when(lead[n] == 1)
            def _():
                force_copies[n].start()
                macro_copies[n].start()

    gap = wrap(lax.broadcasted_iota(jnp.int32, (depth, count), 0) - (base[2:3, :] - 1), depth)
    z_high, z_low = split(pick4(gap, [w[2:3] for w in weights]))
    along[pl.ds(0, depth), :] = z_high
    along[pl.ds(depth, depth), :] = z_low

    comp_of = lane // (window * tiles)
    comps_of = jnp.concatenate([comp_of] * 3, axis=1)

    def mark(ones, s, zrow):
        at = jnp.where(lax.broadcasted_iota(jnp.int32, (depth, run), 0).astype(f32) == zrow, 1.0, 0.0)
        if ones.shape[0] == depth:
            ones[:, pl.ds(s * run, run)] = at.astype(bf16)
            return
        for c in range(3):
            ones[pl.ds(c * depth, depth), pl.ds(s * run, run)] = jnp.where(comp_of == c, at, 0.0).astype(bf16)

    def take_macro(n):
        cells, close, d = plan.edge[n], plan.near[n], sides[n]
        for k in range(4):
            move(
                mr[n],
                [k * len(cells) + i for i in range(len(cells))],
                mac,
                [k * rows + plan.there(c, d) for c in cells],
            )
        return mr[n][pl.ds(plan.macro_rows[n] - 1, 1), :]

    def pop_row(n, q, cell):
        cells, close = plan.edge[n], plan.near[n]
        return 4 * len(cells) + plan.dirs[n].index(q) * len(close) + close.index(cell)

    keep = 1.0 - 1.0 / relax_time
    half = 1.0 - 0.5 / relax_time
    level_row = lax.broadcasted_iota(jnp.int32, (h, 1), 0)

    def population(q, x):
        c = lattice_speeds[q]
        if x < 0 or x >= wx:
            return edge_pops[pl.ds(q * h, h), :]
        value = pops[pl.ds(q * own + x * wy, h), :]
        if c[1] == 1:
            value = jnp.where(level_row == h - 1, mr[4][pl.ds(pop_row(4, q, (x, wy - 1)), 1), :], value)
        if c[1] == -1:
            value = jnp.where(level_row == wy, mr[5][pl.ds(pop_row(5, q, (x, 0)), 1), :], value)
        return value

    def collide(x):
        at = (x + 1) * h
        density = mac[pl.ds(at, h), :]
        force = [grid[pl.ds(k * rows + at, h), :] for k in range(3)]
        inverse = 1.0 / density
        speed = [(mac[pl.ds((k + 1) * rows + at, h), :] + 0.5 * force[k]) * inverse for k in range(3)]
        for k in range(3):
            held = jnp.where((level_row <= wy + 1) | (level_row == h - 1), speed[k], 0.0)
            vel[pl.ds(k * rows + at, h), :] = held
        square = speed[0] * speed[0] + speed[1] * speed[1] + speed[2] * speed[2]
        work = speed[0] * force[0] + speed[1] * force[1] + speed[2] * force[2]
        scaled = density * (1.0 / relax_time)
        level = scaled * (1.0 - 1.5 * square) - (3.0 * half) * work
        carried = [scaled * speed[k] for k in range(3)]
        pushed = [half * force[k] for k in range(3)]
        odd_of = [carried[k] + pushed[k] for k in range(3)]
        even_of = [odd_of[k] + pushed[k] for k in range(3)]
        levels, odds, evens = {}, {}, {}
        for weight in sorted({lattice_weights[q] for q in range(19)}):
            levels[weight] = weight * level
            odds[weight] = [(3.0 * weight) * odd_of[k] for k in range(3)]
            evens[weight] = [(4.5 * weight) * even_of[k] for k in range(3)]
        for first in [0] + list(range(1, 19, 2)):
            pair = [0] if first == 0 else [first, first + 1]
            pair = [q for q in pair if 0 <= x + lattice_speeds[q][0] < wx]
            if not pair:
                continue
            weight = lattice_weights[first]
            even, odd = levels[weight], None
            if first:
                c = lattice_speeds[first]
                even = even + along_speed(c, speed) * along_speed(c, evens[weight])
                odd = along_speed(c, odds[weight])
            for q in pair:
                c = lattice_speeds[q]
                total = even if odd is None else even + odd if q == first else even - odd
                value = keep * population(q, x) + total
                if c[1]:
                    value = pltpu.roll(value, c[1] % h, 0)
                if c[2]:
                    value = pltpu.roll(value, c[2] % depth, 1)
                fresh[pl.ds(q * own + (x + c[0]) * wy, wy), :] = value[0:wy]

    mark(ones_y, 0, zmap)
    arrive(1, (4, 5))
    for s, n in ((1, 4), (2, 5)):
        mark(ones_y, s, take_macro(n))
    arrive(3, (4, 5))
    for n in (4, 5):
        move(fr[n], list(range(plan.force_rows[n])), placed[n], [plan.there(c, sides[n]) for c in plan.force[n]])

    def widen(parts, ones):
        value = transposed_dot(halves(jnp.concatenate(parts, axis=1)), ones[...])
        half_rows = value.shape[0] // 2
        return value[0:half_rows] + value[half_rows:]

    value = widen([comb[...], placed[4][...], placed[5][...]], ones_y)
    for c in range(3):
        grid[pl.ds(c * rows, rows), :] = value[:, c * depth : (c + 1) * depth]
    for x in plan.xs:
        if not plan.late(x):
            collide(x)

    for k, value in enumerate(sample(vel, plane, along, rows, [(left, right - left)])):
        part_sum[pl.ds(8 * k, 8), :] = value

    arrive(1, late)
    for ones, order in ((ones_l, (6, 0, 1)), (ones_r, (7, 2, 3))):
        for s, n in enumerate(order):
            mark(ones, s, take_macro(n))
            for q in plan.dirs[n]:
                close = plan.near[n]
                src = [pop_row(n, q, c) for c in close]
                move(mr[n], src, edge_pops, [q * h + (c[1] - sides[n][1] * wy) % h for c in close])
    arrive(3, late)
    for ones, order, at in ((ones_l, (6, 0, 1), 0), (ones_r, (7, 2, 3), right)):
        for n in order[1:]:
            dst = [plan.there(c, sides[n]) - at for c in plan.force[n]]
            move(fr[n], list(range(plan.force_rows[n])), placed[n], dst)
        parts = jnp.concatenate([fr[order[0]][...], placed[order[1]][...], placed[order[2]][...]], axis=1)
        parts = jnp.concatenate([jnp.where(comps_of == c, parts, 0.0) for c in range(3)], axis=0)
        value = transposed_dot(halves(parts), ones[...])
        for c in range(3):
            here = pl.ds(c * rows + at, 3 * h)
            both = value[3 * h * c : 3 * h * (c + 1)] + value[3 * h * (c + 3) : 3 * h * (c + 4)]
            grid[here, :] = grid[here, :] + both
    for x in plan.xs:
        if plan.late(x):
            collide(x)
    sent = pops.at[pl.ds(0, sum(plan.macro_rows) + sum(plan.force_rows)), :]
    pltpu.make_async_remote_copy(
        src_ref=sent,
        dst_ref=sent,
        send_sem=sems.at[0],
        recv_sem=sems.at[1],
        device_id=peers[0],
        device_id_type=pl.DeviceIdType.MESH,
    ).wait_send()


def finish_kernel(plan, fresh, vel, plane, along, part_sum, fresh_out, sampled_out, sampled, sems):
    h, size = plan.h, fresh.shape[0]
    step = up(size // pieces, 8)
    leave = []
    for i in range(pieces):
        here = pl.ds(i * step, min(step, size - i * step))
        leave.append(pltpu.make_async_copy(fresh.at[here, :], fresh_out.at[here, :], sems.at[i]))
    for copy in leave:
        copy.start()
    leave.append(pltpu.make_async_copy(sampled, sampled_out, sems.at[pieces]))
    for k, value in enumerate(sample(vel, plane, along, plan.rows, [(0, 3 * h), (plan.wx * h, 3 * h)])):
        value = value + part_sum[pl.ds(8 * k, 8), :]
        sampled[k : k + 1, :] = jnp.sum(value, axis=0, keepdims=True)
    leave[-1].start()
    for copy in leave:
        copy.wait()


def solution(mesh):
    nx, ny = mesh.shape["gx"], mesh.shape["gy"]

    def per_device(populations, vert_base, vert_frac, edges, stiffness, rest):
        _, wx, wy, depth = populations.shape
        count, edge_count = vert_base.shape[1], edges.shape[1]
        plan = Plan(wx, wy)
        rows, tiles, h = plan.rows, count // run, plan.h
        macro = [pltpu.VMEM((n, depth), f32) for n in plan.macro_rows]
        force = [pltpu.VMEM((n, run), f32) for n in plan.force_rows]
        scratch = macro + macro + force + force
        scratch += [
            pltpu.VMEM((19 * wx * wy + h, depth), f32),
            pltpu.VMEM((3, count), jnp.int32),
            pltpu.VMEM((3, count), f32),
            pltpu.VMEM((2, edge_count), jnp.int32),
            pltpu.VMEM((edge_count,), f32),
            pltpu.VMEM((3, edge_count), f32),
            pltpu.VMEM((up(4 * tiles, 8), run), f32),
            pltpu.VMEM((8, edge_count), f32),
            pltpu.VMEM((up(4 * tiles, 8), run), f32),
            pltpu.VMEM((4 * rows, depth), f32),
            pltpu.VMEM((3 * rows, depth), f32),
            pltpu.VMEM((rows, run), f32),
            pltpu.VMEM((up(plan.cols, 8), count), f32),
        ]
        scratch += [pltpu.VMEM((rows if n in (4, 5) else 3 * h, run), f32) for n in range(8)]
        scratch += [pltpu.VMEM((n * depth, 3 * run), bf16) for n in (3, 1, 1)]
        scratch += [
            pltpu.VMEM((19 * h, depth), f32),
            pltpu.SemaphoreType.DMA((5,)),
            pltpu.SemaphoreType.DMA((6,)),
            pltpu.SemaphoreType.REGULAR((len(groups),)),
        ]
        vmem = pl.BlockSpec(memory_space=pltpu.VMEM)
        far = pl.BlockSpec(memory_space=pltpu.HBM)

        def exchange(*refs):
            exchange_kernel(plan, nx, ny, *refs)

        def finish(*refs):
            finish_kernel(plan, *refs)

        held = pl.pallas_call(
            exchange,
            out_shape=(
                jax.ShapeDtypeStruct((19 * wx * wy, depth), f32),
                jax.ShapeDtypeStruct((3 * rows, depth), f32),
                jax.ShapeDtypeStruct((rows, count), f32),
                jax.ShapeDtypeStruct((2 * depth, count), bf16),
                jax.ShapeDtypeStruct((24, count), f32),
            ),
            in_specs=[far] * 6,
            out_specs=(vmem,) * 5,
            scratch_shapes=scratch,
            compiler_params=pltpu.CompilerParams(
                collective_id=0, has_side_effects=True, vmem_limit_bytes=24 * 1024 * 1024
            ),
            name="exchange",
        )(
            *[
                pltpu.with_memory_space_constraint(value, pltpu.HBM)
                for value in (
                    populations.reshape(19 * wx * wy, depth),
                    vert_base,
                    vert_frac,
                    edges,
                    stiffness,
                    rest,
                )
            ]
        )
        fresh, sampled = pl.pallas_call(
            finish,
            out_shape=(
                jax.ShapeDtypeStruct((19 * wx * wy, depth), f32),
                jax.ShapeDtypeStruct((3, count), f32),
            ),
            in_specs=[vmem] * 5,
            out_specs=(far, far),
            scratch_shapes=[pltpu.VMEM((3, count), f32), pltpu.SemaphoreType.DMA((pieces + 1,))],
            compiler_params=pltpu.CompilerParams(vmem_limit_bytes=24 * 1024 * 1024),
            name="finish",
        )(*held)
        return fresh.reshape(19, wx, wy, depth), sampled

    placed = (
        P(None, "gx", "gy", None),
        P(None, ("gx", "gy")),
        P(None, ("gx", "gy")),
        P(None, ("gx", "gy")),
        P(("gx", "gy")),
        P(None, ("gx", "gy")),
    )
    return jax.shard_map(
        per_device,
        mesh=mesh,
        in_specs=placed,
        out_specs=(P(None, "gx", "gy", None), P(None, ("gx", "gy"))),
        check_vma=False,
    )
```

```python
import jax
import jax.numpy as jnp
from jax import lax
from jax.experimental import pallas as pl
from jax.experimental.pallas import tpu as pltpu
from jax.sharding import PartitionSpec as P

lattice_speeds = [
    (0, 0, 0),
    (1, 0, 0),
    (-1, 0, 0),
    (0, 1, 0),
    (0, -1, 0),
    (0, 0, 1),
    (0, 0, -1),
    (1, 1, 0),
    (-1, -1, 0),
    (1, -1, 0),
    (-1, 1, 0),
    (1, 0, 1),
    (-1, 0, -1),
    (1, 0, -1),
    (-1, 0, 1),
    (0, 1, 1),
    (0, -1, -1),
    (0, 1, -1),
    (0, -1, 1),
]
lattice_weights = [1.0 / 3.0] + [1.0 / 18.0] * 6 + [1.0 / 36.0] * 12
relax_time = 0.9
run = 128
window = 8
pieces = 1
sides = [(1, 1), (1, -1), (-1, 1), (-1, -1), (0, 1), (0, -1), (1, 0), (-1, 0)]
groups = [(0, 1, 6), (2, 3, 7), (4,), (5,)]
f32, bf16 = jnp.float32, jnp.bfloat16


def outer_weight(r):
    return (5.0 - 2.0 * r - jnp.sqrt(-7.0 + 12.0 * r - 4.0 * r * r)) / 8.0


def inner_weight(r):
    return (3.0 - 2.0 * r + jnp.sqrt(1.0 + 4.0 * r - 4.0 * r * r)) / 8.0


def up(n, m):
    return (n + m - 1) // m * m


class Plan:
    def __init__(self, wx, wy):
        self.wx, self.wy, self.own = wx, wy, wx * wy
        self.h = up(wy + 3, 8)
        self.cols = wx + 3
        self.rows = up(self.cols * self.h, 16)
        self.xs = list(range(-1, wx + 2))

        def span(d, w):
            return {0: list(range(-1, w + 2)), 1: [w - 1, w, w + 1], -1: [-1, 0, 1]}[d]

        def edge(d, w):
            return {0: list(range(w)), 1: [w - 1], -1: [0, 1]}[d]

        def near(d, w):
            return {0: list(range(w)), 1: [w - 1], -1: [0]}[d]

        def cells(d, pick):
            xs, ys = pick(d[0], wx), pick(d[1], wy)
            if d[0]:
                return [(x, y) for x in xs for y in ys]
            return [(x, y) for y in ys for x in xs]

        self.edge = [cells(d, edge) for d in sides]
        self.near = [cells(d, near) for d in sides]
        self.force = [cells(d, span) for d in sides]
        self.dirs = [
            [
                q
                for q, c in enumerate(lattice_speeds)
                if (not d[0] or c[0] == d[0]) and (not d[1] or c[1] == d[1])
            ]
            for d in sides
        ]
        self.macro_rows = [
            4 * len(e) + len(q) * len(n) + 1 for e, q, n in zip(self.edge, self.dirs, self.near)
        ]
        self.force_rows = [3 * self.h if d[1] == 0 else len(c) for d, c in zip(sides, self.force)]

    def row(self, x, y):
        return (x + 1) * self.h + y % self.h

    def there(self, cell, d):
        return self.row(cell[0] - d[0] * self.wx, cell[1] - d[1] * self.wy)

    def late(self, x):
        return x < 2 or x > self.wx - 2


def runs(src, dst):
    out, i = [], 0
    while i < len(src):
        n, a, b = 1, 1, 1
        if i + 1 < len(src) and src[i + 1] > src[i] and dst[i + 1] > dst[i]:
            a, b = src[i + 1] - src[i], dst[i + 1] - dst[i]
            n = 2
            while i + n < len(src) and src[i + n] - src[i + n - 1] == a and dst[i + n] - dst[i + n - 1] == b:
                n += 1
        out.append((src[i], a, dst[i], b, n))
        i += n
    return out


def ds(start, n, stride):
    return pl.ds(start, n, stride=stride) if stride > 1 else pl.ds(start, n)


def move(src_ref, src, dst_ref, dst):
    for s, a, d, b, n in runs(src, dst):
        dst_ref[ds(d, n, b), :] = src_ref[ds(s, n, a), :]


def split(value):
    high = value.astype(bf16)
    return high, (value - high.astype(f32)).astype(bf16)


def halves(value):
    return jnp.concatenate(split(value), axis=0)


def pick4(delta, weights):
    out = jnp.zeros(delta.shape, f32)
    for k in range(4):
        out = jnp.where(delta == k, weights[k], out)
    return out


def wrap(value, depth):
    value = jnp.where(value < 0, value + depth, value)
    return jnp.where(value >= depth, value - depth, value)


def along_speed(c, vector):
    total = None
    for k in range(3):
        if c[k]:
            term = vector[k] if c[k] > 0 else -vector[k]
            total = term if total is None else total + term
    return total


def transposed_dot(a, b):
    return lax.dot_general(a, b, (((1,), (1,)), ((), ())), preferred_element_type=f32)


def sample(vel, plane, along, rows, spans):
    flat = jnp.concatenate([plane[pl.ds(a, n), :] for a, n in spans], axis=0)
    value = jnp.concatenate([vel[pl.ds(k * rows + a, n), :] for k in range(3) for a, n in spans], axis=0)
    v_high, v_low = split(value)
    value = jnp.dot(jnp.concatenate([v_high, v_low, v_high], axis=1), along[...], preferred_element_type=f32)
    size = flat.shape[0]
    out = []
    for k in range(3):
        both = value[k * size : (k + 1) * size] * flat
        acc = both[0:8]
        for r in range(8, size, 8):
            acc = acc + both[r : r + 8]
        out.append(acc)
    return out


def exchange_kernel(plan, nx, ny, *refs):
    wx, wy, h, rows, own = plan.wx, plan.wy, plan.h, plan.rows, plan.own
    sources, scratch = refs[0:6], refs[11:]
    fresh, vel, plane, along, part_sum = refs[6:11]
    ms, mr, fs, fr = scratch[0:8], scratch[8:16], scratch[16:24], scratch[24:32]
    (pops, base, frac, edges, stiff, rest, pos, pull, mem, mac, grid, comb, px_ref) = scratch[32:45]
    placed = scratch[45:53]
    ones_y, ones_l, ones_r, edge_pops, sems, load_sems, ready = scratch[53:]
    depth = pops.shape[1]
    load_into = (pops.at[pl.ds(0, 19 * own), :], base, frac, edges, stiff, rest)
    loads_in = [pltpu.make_async_copy(sources[n], load_into[n], load_sems.at[min(n, 1)]) for n in range(6)]
    for n in (3, 2, 1, 5, 4, 0):
        loads_in[n].start()
    count = base.shape[1]
    edge_count = edges.shape[1]
    tiles = count // run
    ix, iy = lax.axis_index("gx"), lax.axis_index("gy")
    peers = [(lax.rem(ix + dx + nx, nx), lax.rem(iy + dy + ny, ny)) for dx, dy in sides]

    def rank(px, py):
        return px * ny + py

    key = rank(ix, iy)
    lead = [(key < rank(px, py)).astype(jnp.int32) for px, py in peers]
    led = [sum(lead[n] for n in g) for g in groups]
    barrier = pltpu.get_barrier_semaphore()

    def hail(sem, n):
        pl.semaphore_signal(sem, inc=1, device_id=peers[n], device_id_type=pl.DeviceIdType.MESH)

    for n in range(8):

        @pl.when(lead[n] == 1)
        def _():
            hail(barrier, n)

    def copies(src, dst, kind):
        return [
            pltpu.make_async_remote_copy(
                src_ref=src[n],
                dst_ref=dst[n],
                send_sem=sems.at[0],
                recv_sem=sems.at[kind + (0 if n in (4, 5) else 1)],
                device_id=peers[n],
                device_id_type=pl.DeviceIdType.MESH,
            )
            for n in range(8)
        ]

    first_col = {1: wx, -1: 0}
    outgoing = list(fs)
    for n in (6, 7):
        outgoing[n] = comb.at[pl.ds(first_col[sides[n][0]] * h, 3 * h), :]
    macro_copies = copies(ms, mr, 1)
    force_copies = copies(outgoing, fr, 3)

    def arrive(kind, which):
        lengths = plan.macro_rows if kind == 1 else plan.force_rows
        all_of = pops.at[pl.ds(0, sum(lengths[n] for n in which)), :]
        pltpu.make_async_remote_copy(
            src_ref=all_of,
            dst_ref=all_of,
            send_sem=sems.at[0],
            recv_sem=sems.at[kind + (0 if 4 in which else 1)],
            device_id=peers[0],
            device_id_type=pl.DeviceIdType.MESH,
        ).wait_recv()

    zeros = jnp.zeros((8, run), f32)
    comb[...] = jnp.zeros(comb.shape, f32)
    pos[...] = jnp.zeros(pos.shape, f32)
    pull[...] = jnp.zeros(pull.shape, f32)
    for ref in placed:
        ref[...] = jnp.zeros(ref.shape, f32)
    for n in (3, 2, 1, 5, 4):
        loads_in[n].wait()

    moved = frac[...]
    weights = [
        outer_weight(1.0 + moved),
        inner_weight(moved),
        inner_weight(1.0 - moved),
        outer_weight(2.0 - moved),
    ]
    lane = lax.broadcasted_iota(jnp.int32, (1, run), 1)
    slot = lax.rem(lane, window)
    of_tile = lax.rem(lane // window, tiles)
    start_of = jnp.zeros((1, run), jnp.int32)
    offsets = []
    for t in range(tiles):
        z = base[2:3, t * run : (t + 1) * run]
        gap = z - z[0:1, 0:1]
        gap = jnp.where(gap > depth // 2, gap - depth, gap)
        gap = jnp.where(gap < -(depth // 2), gap + depth, gap)
        low = jnp.min(gap, axis=1, keepdims=True)
        offsets.append(gap - low)
        start_of = jnp.where(of_tile == t, z[0:1, 0:1] + low - 1, start_of)
    zmap = wrap(start_of + slot, depth).astype(f32)
    offset = jnp.concatenate(offsets, axis=1)
    reach_z = pick4(lax.broadcasted_iota(jnp.int32, (window, count), 0) - offset, [w[2:3] for w in weights])

    pairs = up(tiles, 2) // 2
    ends = edges[...]
    tail = jnp.bitwise_and(ends[0:1], run - 1)
    head = jnp.bitwise_and(ends[1:2], run - 1)
    group = lax.shift_right_logical(ends[0:1], run.bit_length() - 1)
    whole = base[...].astype(f32) + moved
    for t in range(tiles):
        pos[pl.ds(4 * t, 3), :] = whole[:, t * run : (t + 1) * run]
    for k in (0, 4):
        pull[pl.ds(k, 3), :] = rest[...]
    half_of = lax.broadcasted_iota(jnp.int32, (8, edge_count), 0) // 4
    mine = [group == 2 * p + half_of for p in range(pairs)]
    tables = [pos[pl.ds(8 * p, 8), :] for p in range(pairs)]
    pieces_of = []
    for k in range(0, edge_count, run):
        cols = slice(k, k + run)
        heads_at, tails_at = (jnp.broadcast_to(value[:, cols], (8, run)) for value in (head, tail))
        piece = jnp.zeros((8, run), f32)
        fronts = [jnp.take_along_axis(table, heads_at, axis=1) for table in tables]
        backs = [jnp.take_along_axis(table, tails_at, axis=1) for table in tables]
        for p in range(pairs):
            piece = jnp.where(mine[p][:, cols], fronts[p] - backs[p], piece)
        pieces_of.append(piece)
    diff = jnp.concatenate(pieces_of, axis=1)
    stretch = stiff[...].reshape(1, edge_count) * (diff - pull[...])
    terms = jnp.concatenate([jnp.where(mine[p], stretch, 0.0) for p in range(pairs)], axis=0)
    spot = lax.broadcasted_iota(jnp.int32, (run, edge_count), 0).astype(f32).astype(bf16)
    one, none = jnp.ones((), bf16), jnp.zeros((), bf16)
    heads, tails = (value.astype(f32).astype(bf16) for value in (head, tail))
    hot = jnp.where(spot == heads, one, jnp.where(spot == tails, -one, none))
    part = 8 * pairs
    summed = transposed_dot(halves(terms), hot)
    mem[...] = -(summed[0:part] + summed[part : 2 * part])

    def moments(r):
        totals = [None] * 4
        for q, c in enumerate(lattice_speeds):
            value = pops[pl.ds(q * own + r, 8), :]
            for k, sign in enumerate((1,) + c):
                if sign:
                    term = value if sign > 0 else -value
                    totals[k] = term if totals[k] is None else totals[k] + term
        for k in range(4):
            for i in range(0, 8, wy):
                mac[pl.ds(k * rows + plan.row((r + i) // wy, 0), wy), :] = totals[k][i : i + wy]

    def pack(n):
        cells, close = plan.edge[n], plan.near[n]
        for k in range(4):
            move(
                mac,
                [k * rows + plan.row(x, y) for x, y in cells],
                ms[n],
                [k * len(cells) + i for i in range(len(cells))],
            )
        for s, q in enumerate(plan.dirs[n]):
            first = 4 * len(cells) + s * len(close)
            move(pops, [q * own + x * wy + y for x, y in close], ms[n], [first + i for i in range(len(close))])
        ms[n][pl.ds(plan.macro_rows[n] - 1, 1), :] = zmap

    late = (0, 1, 6, 2, 3, 7)

    bx = base[0:1, :] - ix * wx - 1
    by = base[1:2, :] - iy * wy - 1
    i = lax.broadcasted_iota(jnp.int32, (px_ref.shape[0], 1), 0)
    px_ref[...] = pick4(i - 1 - bx, [w[0:1] for w in weights])
    i = lax.broadcasted_iota(jnp.int32, (h, 1), 0)
    y = jnp.where(i == h - 1, -1, jnp.where(i > wy + 1, -100, i))
    py = pick4(y - by, [w[1:2] for w in weights])
    big, small = [], []
    for c in range(3):
        for t in range(tiles):
            cols = slice(t * run, (t + 1) * run)
            block = reach_z[:, cols] * mem[pl.ds(4 * t + c, 1), :]
            rounded = block.astype(bf16).astype(f32)
            for out, value in ((big, rounded), (small, block - rounded)):
                out.append(jnp.concatenate([value if t == s else zeros for s in range(tiles)], axis=1))
    pad = [jnp.zeros((run - 3 * tiles * window, count), f32)]
    source = jnp.concatenate(big + pad + small + pad, axis=0).astype(bf16)

    def spread(spans):
        for a, n in spans:
            for k in range(a // h, (a + n) // h):
                plane[pl.ds(k * h, h), :] = px_ref[pl.ds(k, 1), :] * py
        flat = jnp.concatenate([plane[pl.ds(a, n), :] for a, n in spans], axis=0)
        size = flat.shape[0]
        value = transposed_dot(halves(flat), source)
        value = value[0:size] + value[size : 2 * size]
        value = value[:, 0:run] + value[:, run : 2 * run]
        done = 0
        for a, n in spans:
            comb[pl.ds(a, n), :] = value[done : done + n]
            done += n

    left, right = 3 * h, wx * h
    spread([(0, left), (right, 3 * h)])
    for n in range(4):
        move(comb, [plan.row(x, y) for x, y in plan.force[n]], fs[n], list(range(plan.force_rows[n])))
    loads_in[0].wait()
    ends_of = sorted({x * wy // 8 * 8 for x in (0, 1, wx - 1)})
    for r in ends_of:
        moments(r)
    for n in late:
        pack(n)

    greetings = 8 - sum(lead)

    @pl.when(greetings > 0)
    def _():
        pl.semaphore_wait(barrier, greetings)

    for n in range(8):
        back = sides.index((-sides[n][0], -sides[n][1]))
        slot_of = [i for i, g in enumerate(groups) if back in g][0]

        @pl.when(lead[n] == 0)
        def _():
            hail(ready.at[slot_of], n)

    for n in late:

        @pl.when(lead[n] == 0)
        def _():
            macro_copies[n].start()
            force_copies[n].start()

    for r in range(0, own, 8):
        if r not in ends_of:
            moments(r)
    for n in (4, 5):
        pack(n)

    for n in (4, 5):

        @pl.when(lead[n] == 0)
        def _():
            macro_copies[n].start()

    spread([(left, right - left)])
    for n in (4, 5):
        move(comb, [plan.row(x, y) for x, y in plan.force[n]], fs[n], list(range(plan.force_rows[n])))
    for n in (4, 5):

        @pl.when(lead[n] == 0)
        def _():
            force_copies[n].start()

    gap = wrap(lax.broadcasted_iota(jnp.int32, (depth, count), 0) - (base[2:3, :] - 1), depth)
    z_high, z_low = split(pick4(gap, [w[2:3] for w in weights]))
    for k, value in enumerate((z_high, z_high, z_low)):
        along[pl.ds(k * depth, depth), :] = value

    for i in (2, 3, 0, 1):

        @pl.when(led[i] > 0)
        def _():
            pl.semaphore_wait(ready.at[i], led[i])

        for n in groups[i]:

            @pl.when(lead[n] == 1)
            def _():
                force_copies[n].start()
                macro_copies[n].start()

    comp_of = lane // (window * tiles)
    comps_of = jnp.concatenate([comp_of] * 3, axis=1)

    def mark(ones, s, zrow):
        at = jnp.where(lax.broadcasted_iota(jnp.int32, (depth, run), 0).astype(f32) == zrow, 1.0, 0.0)
        if ones.shape[0] == depth:
            ones[:, pl.ds(s * run, run)] = at.astype(bf16)
            return
        for c in range(3):
            ones[pl.ds(c * depth, depth), pl.ds(s * run, run)] = jnp.where(comp_of == c, at, 0.0).astype(bf16)

    def take_macro(n):
        cells, close, d = plan.edge[n], plan.near[n], sides[n]
        for k in range(4):
            move(
                mr[n],
                [k * len(cells) + i for i in range(len(cells))],
                mac,
                [k * rows + plan.there(c, d) for c in cells],
            )
        return mr[n][pl.ds(plan.macro_rows[n] - 1, 1), :]

    def pop_row(n, q, cell):
        cells, close = plan.edge[n], plan.near[n]
        return 4 * len(cells) + plan.dirs[n].index(q) * len(close) + close.index(cell)

    keep = 1.0 - 1.0 / relax_time
    half = 1.0 - 0.5 / relax_time
    level_row = lax.broadcasted_iota(jnp.int32, (h, 1), 0)

    def population(q, x):
        c = lattice_speeds[q]
        if x < 0 or x >= wx:
            return edge_pops[pl.ds(q * h, h), :]
        value = pops[pl.ds(q * own + x * wy, h), :]
        if c[1] == 1:
            value = jnp.where(level_row == h - 1, mr[4][pl.ds(pop_row(4, q, (x, wy - 1)), 1), :], value)
        if c[1] == -1:
            value = jnp.where(level_row == wy, mr[5][pl.ds(pop_row(5, q, (x, 0)), 1), :], value)
        return value

    def collide(x):
        at = (x + 1) * h
        density = mac[pl.ds(at, h), :]
        force = [grid[pl.ds(k * rows + at, h), :] for k in range(3)]
        inverse = 1.0 / density
        speed = [(mac[pl.ds((k + 1) * rows + at, h), :] + 0.5 * force[k]) * inverse for k in range(3)]
        for k in range(3):
            held = jnp.where((level_row <= wy + 1) | (level_row == h - 1), speed[k], 0.0)
            vel[pl.ds(k * rows + at, h), :] = held
        square = speed[0] * speed[0] + speed[1] * speed[1] + speed[2] * speed[2]
        work = speed[0] * force[0] + speed[1] * force[1] + speed[2] * force[2]
        scaled = density * (1.0 / relax_time)
        level = scaled * (1.0 - 1.5 * square) - (3.0 * half) * work
        carried = [scaled * speed[k] for k in range(3)]
        pushed = [half * force[k] for k in range(3)]
        odd_of = [carried[k] + pushed[k] for k in range(3)]
        even_of = [odd_of[k] + pushed[k] for k in range(3)]
        levels, odds, evens = {}, {}, {}
        for weight in sorted({lattice_weights[q] for q in range(19)}):
            levels[weight] = weight * level
            odds[weight] = [(3.0 * weight) * odd_of[k] for k in range(3)]
            evens[weight] = [(4.5 * weight) * even_of[k] for k in range(3)]
        for first in [0] + list(range(1, 19, 2)):
            pair = [0] if first == 0 else [first, first + 1]
            pair = [q for q in pair if 0 <= x + lattice_speeds[q][0] < wx]
            if not pair:
                continue
            weight = lattice_weights[first]
            even, odd = levels[weight], None
            if first:
                c = lattice_speeds[first]
                even = even + along_speed(c, speed) * along_speed(c, evens[weight])
                odd = along_speed(c, odds[weight])
            for q in pair:
                c = lattice_speeds[q]
                total = even if odd is None else even + odd if q == first else even - odd
                value = keep * population(q, x) + total
                if c[1]:
                    value = pltpu.roll(value, c[1] % h, 0)
                if c[2]:
                    value = pltpu.roll(value, c[2] % depth, 1)
                fresh[pl.ds(q * own + (x + c[0]) * wy, wy), :] = value[0:wy]

    mark(ones_y, 0, zmap)
    arrive(1, (4, 5))
    for s, n in ((1, 4), (2, 5)):
        mark(ones_y, s, take_macro(n))
    arrive(3, (4, 5))
    for n in (4, 5):
        move(fr[n], list(range(plan.force_rows[n])), placed[n], [plan.there(c, sides[n]) for c in plan.force[n]])

    def widen(parts, ones):
        value = transposed_dot(halves(jnp.concatenate(parts, axis=1)), ones[...])
        half_rows = value.shape[0] // 2
        return value[0:half_rows] + value[half_rows:]

    value = widen([comb[...], placed[4][...], placed[5][...]], ones_y)
    for c in range(3):
        grid[pl.ds(c * rows, rows), :] = value[:, c * depth : (c + 1) * depth]
    for x in plan.xs:
        if not plan.late(x):
            collide(x)

    for k, value in enumerate(sample(vel, plane, along, rows, [(left, right - left)])):
        part_sum[pl.ds(8 * k, 8), :] = value

    arrive(1, late)
    for ones, order in ((ones_l, (6, 0, 1)), (ones_r, (7, 2, 3))):
        for s, n in enumerate(order):
            mark(ones, s, take_macro(n))
            for q in plan.dirs[n]:
                close = plan.near[n]
                src = [pop_row(n, q, c) for c in close]
                move(mr[n], src, edge_pops, [q * h + (c[1] - sides[n][1] * wy) % h for c in close])
    arrive(3, late)
    for ones, order, at in ((ones_l, (6, 0, 1), 0), (ones_r, (7, 2, 3), right)):
        for n in order[1:]:
            dst = [plan.there(c, sides[n]) - at for c in plan.force[n]]
            move(fr[n], list(range(plan.force_rows[n])), placed[n], dst)
        parts = jnp.concatenate([fr[order[0]][...], placed[order[1]][...], placed[order[2]][...]], axis=1)
        rounded = parts.astype(bf16).astype(f32)
        both = (rounded, parts - rounded)
        parts = jnp.concatenate([jnp.where(comps_of == c, value, 0.0) for value in both for c in range(3)], axis=0)
        value = transposed_dot(parts.astype(bf16), ones[...])
        for c in range(3):
            here = pl.ds(c * rows + at, 3 * h)
            both = value[3 * h * c : 3 * h * (c + 1)] + value[3 * h * (c + 3) : 3 * h * (c + 4)]
            grid[here, :] = grid[here, :] + both
    for x in plan.xs:
        if plan.late(x):
            collide(x)
    sent = pops.at[pl.ds(0, sum(plan.macro_rows) + sum(plan.force_rows)), :]
    pltpu.make_async_remote_copy(
        src_ref=sent,
        dst_ref=sent,
        send_sem=sems.at[0],
        recv_sem=sems.at[1],
        device_id=peers[0],
        device_id_type=pl.DeviceIdType.MESH,
    ).wait_send()


def finish_kernel(plan, fresh, vel, plane, along, part_sum, fresh_out, sampled_out, sampled, sems):
    h, size = plan.h, fresh.shape[0]
    step = up(size // pieces, 8)
    leave = []
    for i in range(pieces):
        here = pl.ds(i * step, min(step, size - i * step))
        leave.append(pltpu.make_async_copy(fresh.at[here, :], fresh_out.at[here, :], sems.at[i]))
    for copy in leave:
        copy.start()
    leave.append(pltpu.make_async_copy(sampled, sampled_out, sems.at[pieces]))
    for k, value in enumerate(sample(vel, plane, along, plan.rows, [(0, 3 * h), (plan.wx * h, 3 * h)])):
        value = value + part_sum[pl.ds(8 * k, 8), :]
        sampled[k : k + 1, :] = jnp.sum(value, axis=0, keepdims=True)
    leave[-1].start()
    for copy in leave:
        copy.wait()


def solution(mesh):
    nx, ny = mesh.shape["gx"], mesh.shape["gy"]

    def per_device(populations, vert_base, vert_frac, edges, stiffness, rest):
        _, wx, wy, depth = populations.shape
        count, edge_count = vert_base.shape[1], edges.shape[1]
        plan = Plan(wx, wy)
        rows, tiles, h = plan.rows, count // run, plan.h
        macro = [pltpu.VMEM((n, depth), f32) for n in plan.macro_rows]
        force = [pltpu.VMEM((n, run), f32) for n in plan.force_rows]
        scratch = macro + macro + force + force
        scratch += [
            pltpu.VMEM((19 * wx * wy + h, depth), f32),
            pltpu.VMEM((3, count), jnp.int32),
            pltpu.VMEM((3, count), f32),
            pltpu.VMEM((2, edge_count), jnp.int32),
            pltpu.VMEM((edge_count,), f32),
            pltpu.VMEM((3, edge_count), f32),
            pltpu.VMEM((up(4 * tiles, 8), run), f32),
            pltpu.VMEM((8, edge_count), f32),
            pltpu.VMEM((up(4 * tiles, 8), run), f32),
            pltpu.VMEM((4 * rows, depth), f32),
            pltpu.VMEM((3 * rows, depth), f32),
            pltpu.VMEM((rows, run), f32),
            pltpu.VMEM((up(plan.cols, 8), count), f32),
        ]
        scratch += [pltpu.VMEM((rows if n in (4, 5) else 3 * h, run), f32) for n in range(8)]
        scratch += [pltpu.VMEM((n * depth, 3 * run), bf16) for n in (3, 1, 1)]
        scratch += [
            pltpu.VMEM((19 * h, depth), f32),
            pltpu.SemaphoreType.DMA((5,)),
            pltpu.SemaphoreType.DMA((2,)),
            pltpu.SemaphoreType.REGULAR((len(groups),)),
        ]
        vmem = pl.BlockSpec(memory_space=pltpu.VMEM)
        far = pl.BlockSpec(memory_space=pltpu.HBM)

        def exchange(*refs):
            exchange_kernel(plan, nx, ny, *refs)

        def finish(*refs):
            finish_kernel(plan, *refs)

        held = pl.pallas_call(
            exchange,
            out_shape=(
                jax.ShapeDtypeStruct((19 * wx * wy, depth), f32),
                jax.ShapeDtypeStruct((3 * rows, depth), f32),
                jax.ShapeDtypeStruct((rows, count), f32),
                jax.ShapeDtypeStruct((3 * depth, count), bf16),
                jax.ShapeDtypeStruct((24, count), f32),
            ),
            in_specs=[far] * 6,
            out_specs=(vmem,) * 5,
            scratch_shapes=scratch,
            compiler_params=pltpu.CompilerParams(
                collective_id=0, has_side_effects=True, vmem_limit_bytes=24 * 1024 * 1024
            ),
            name="exchange",
        )(
            *[
                pltpu.with_memory_space_constraint(value, pltpu.HBM)
                for value in (
                    populations.reshape(19 * wx * wy, depth),
                    vert_base,
                    vert_frac,
                    edges,
                    stiffness,
                    rest,
                )
            ]
        )
        fresh, sampled = pl.pallas_call(
            finish,
            out_shape=(
                jax.ShapeDtypeStruct((19 * wx * wy, depth), f32),
                jax.ShapeDtypeStruct((3, count), f32),
            ),
            in_specs=[vmem] * 5,
            out_specs=(far, far),
            scratch_shapes=[pltpu.VMEM((3, count), f32), pltpu.SemaphoreType.DMA((pieces + 1,))],
            compiler_params=pltpu.CompilerParams(vmem_limit_bytes=24 * 1024 * 1024),
            name="finish",
        )(*held)
        return fresh.reshape(19, wx, wy, depth), sampled

    placed = (
        P(None, "gx", "gy", None),
        P(None, ("gx", "gy")),
        P(None, ("gx", "gy")),
        P(None, ("gx", "gy")),
        P(("gx", "gy")),
        P(None, ("gx", "gy")),
    )
    return jax.shard_map(
        per_device,
        mesh=mesh,
        in_specs=placed,
        out_specs=(P(None, "gx", "gy", None), P(None, ("gx", "gy"))),
        check_vma=False,
    )
```

```python
import jax
import jax.numpy as jnp
from jax import lax
from jax.experimental import pallas as pl
from jax.experimental.pallas import tpu as pltpu
from jax.sharding import PartitionSpec as P

lattice_speeds = [
    (0, 0, 0),
    (1, 0, 0),
    (-1, 0, 0),
    (0, 1, 0),
    (0, -1, 0),
    (0, 0, 1),
    (0, 0, -1),
    (1, 1, 0),
    (-1, -1, 0),
    (1, -1, 0),
    (-1, 1, 0),
    (1, 0, 1),
    (-1, 0, -1),
    (1, 0, -1),
    (-1, 0, 1),
    (0, 1, 1),
    (0, -1, -1),
    (0, 1, -1),
    (0, -1, 1),
]
lattice_weights = [1.0 / 3.0] + [1.0 / 18.0] * 6 + [1.0 / 36.0] * 12
relax_time = 0.9
run = 128
window = 8
pieces = 1
sides = [(1, 1), (1, -1), (-1, 1), (-1, -1), (0, 1), (0, -1), (1, 0), (-1, 0)]
groups = [(0, 1, 6), (2, 3, 7), (4,), (5,)]
f32, bf16 = jnp.float32, jnp.bfloat16


def outer_weight(r):
    return (5.0 - 2.0 * r - jnp.sqrt(-7.0 + 12.0 * r - 4.0 * r * r)) / 8.0


def inner_weight(r):
    return (3.0 - 2.0 * r + jnp.sqrt(1.0 + 4.0 * r - 4.0 * r * r)) / 8.0


def up(n, m):
    return (n + m - 1) // m * m


class Plan:
    def __init__(self, wx, wy):
        self.wx, self.wy, self.own = wx, wy, wx * wy
        self.h = up(wy + 3, 8)
        self.cols = wx + 3
        self.rows = up(self.cols * self.h, 16)
        self.xs = list(range(-1, wx + 2))

        def span(d, w):
            return {0: list(range(-1, w + 2)), 1: [w - 1, w, w + 1], -1: [-1, 0, 1]}[d]

        def edge(d, w):
            return {0: list(range(w)), 1: [w - 1], -1: [0, 1]}[d]

        def near(d, w):
            return {0: list(range(w)), 1: [w - 1], -1: [0]}[d]

        def cells(d, pick):
            xs, ys = pick(d[0], wx), pick(d[1], wy)
            if d[0]:
                return [(x, y) for x in xs for y in ys]
            return [(x, y) for y in ys for x in xs]

        self.edge = [cells(d, edge) for d in sides]
        self.near = [cells(d, near) for d in sides]
        self.force = [cells(d, span) for d in sides]
        self.dirs = [
            [
                q
                for q, c in enumerate(lattice_speeds)
                if (not d[0] or c[0] == d[0]) and (not d[1] or c[1] == d[1])
            ]
            for d in sides
        ]
        self.macro_rows = [
            4 * len(e) + len(q) * len(n) + 1 for e, q, n in zip(self.edge, self.dirs, self.near)
        ]
        self.force_rows = [3 * self.h if d[1] == 0 else len(c) for d, c in zip(sides, self.force)]

    def row(self, x, y):
        return (x + 1) * self.h + y % self.h

    def there(self, cell, d):
        return self.row(cell[0] - d[0] * self.wx, cell[1] - d[1] * self.wy)

    def late(self, x):
        return x < 2 or x > self.wx - 2


def runs(src, dst):
    out, i = [], 0
    while i < len(src):
        n, a, b = 1, 1, 1
        if i + 1 < len(src) and src[i + 1] > src[i] and dst[i + 1] > dst[i]:
            a, b = src[i + 1] - src[i], dst[i + 1] - dst[i]
            n = 2
            while i + n < len(src) and src[i + n] - src[i + n - 1] == a and dst[i + n] - dst[i + n - 1] == b:
                n += 1
        out.append((src[i], a, dst[i], b, n))
        i += n
    return out


def ds(start, n, stride):
    return pl.ds(start, n, stride=stride) if stride > 1 else pl.ds(start, n)


def move(src_ref, src, dst_ref, dst):
    for s, a, d, b, n in runs(src, dst):
        dst_ref[ds(d, n, b), :] = src_ref[ds(s, n, a), :]


def split(value):
    high = value.astype(bf16)
    return high, (value - high.astype(f32)).astype(bf16)


def halves(value):
    return jnp.concatenate(split(value), axis=0)


def pick4(delta, weights):
    out = jnp.zeros(delta.shape, f32)
    for k in range(4):
        out = jnp.where(delta == k, weights[k], out)
    return out


def wrap(value, depth):
    value = jnp.where(value < 0, value + depth, value)
    return jnp.where(value >= depth, value - depth, value)


def along_speed(c, vector):
    total = None
    for k in range(3):
        if c[k]:
            term = vector[k] if c[k] > 0 else -vector[k]
            total = term if total is None else total + term
    return total


def transposed_dot(a, b):
    return lax.dot_general(a, b, (((1,), (1,)), ((), ())), preferred_element_type=f32)


def sample(vel, plane, along, rows, spans):
    flat = jnp.concatenate([plane[pl.ds(a, n), :] for a, n in spans], axis=0)
    value = jnp.concatenate([vel[pl.ds(k * rows + a, n), :] for k in range(3) for a, n in spans], axis=0)
    v_high, v_low = split(value)
    value = jnp.dot(jnp.concatenate([v_high, v_low, v_high], axis=1), along[...], preferred_element_type=f32)
    size = flat.shape[0]
    out = []
    for k in range(3):
        both = value[k * size : (k + 1) * size] * flat
        acc = both[0:8]
        for r in range(8, size, 8):
            acc = acc + both[r : r + 8]
        out.append(acc)
    return out


def exchange_kernel(plan, nx, ny, *refs):
    wx, wy, h, rows, own = plan.wx, plan.wy, plan.h, plan.rows, plan.own
    sources, scratch = refs[0:6], refs[11:]
    fresh, vel, plane, along, part_sum = refs[6:11]
    ms, mr, fs, fr = scratch[0:8], scratch[8:16], scratch[16:24], scratch[24:32]
    (pops, base, frac, edges, stiff, rest, pos, pull, mem, mac, grid, comb, px_ref) = scratch[32:45]
    placed = scratch[45:53]
    ones_y, ones_l, ones_r, edge_pops, sems, load_sems, ready = scratch[53:]
    depth = pops.shape[1]
    load_into = (pops.at[pl.ds(0, 19 * own), :], base, frac, edges, stiff, rest)
    loads_in = [pltpu.make_async_copy(sources[n], load_into[n], load_sems.at[min(n, 1)]) for n in range(6)]
    for n in (3, 2, 1, 5, 4, 0):
        loads_in[n].start()
    count = base.shape[1]
    edge_count = edges.shape[1]
    tiles = count // run
    ix, iy = lax.axis_index("gx"), lax.axis_index("gy")
    peers = [(lax.rem(ix + dx + nx, nx), lax.rem(iy + dy + ny, ny)) for dx, dy in sides]

    def rank(px, py):
        return px * ny + py

    key = rank(ix, iy)
    lead = [(key < rank(px, py)).astype(jnp.int32) for px, py in peers]
    led = [sum(lead[n] for n in g) for g in groups]
    barrier = pltpu.get_barrier_semaphore()

    def hail(sem, n):
        pl.semaphore_signal(sem, inc=1, device_id=peers[n], device_id_type=pl.DeviceIdType.MESH)

    for n in range(8):

        @pl.when(lead[n] == 1)
        def _():
            hail(barrier, n)

    def copies(src, dst, kind):
        return [
            pltpu.make_async_remote_copy(
                src_ref=src[n],
                dst_ref=dst[n],
                send_sem=sems.at[0],
                recv_sem=sems.at[kind + (0 if n in (4, 5) else 1)],
                device_id=peers[n],
                device_id_type=pl.DeviceIdType.MESH,
            )
            for n in range(8)
        ]

    first_col = {1: wx, -1: 0}
    outgoing = list(fs)
    for n in (6, 7):
        outgoing[n] = comb.at[pl.ds(first_col[sides[n][0]] * h, 3 * h), :]
    macro_copies = copies(ms, mr, 1)
    force_copies = copies(outgoing, fr, 3)

    def arrive(kind, which):
        lengths = plan.macro_rows if kind == 1 else plan.force_rows
        all_of = pops.at[pl.ds(0, sum(lengths[n] for n in which)), :]
        pltpu.make_async_remote_copy(
            src_ref=all_of,
            dst_ref=all_of,
            send_sem=sems.at[0],
            recv_sem=sems.at[kind + (0 if 4 in which else 1)],
            device_id=peers[0],
            device_id_type=pl.DeviceIdType.MESH,
        ).wait_recv()

    zeros = jnp.zeros((8, run), f32)
    comb[...] = jnp.zeros(comb.shape, f32)
    pos[...] = jnp.zeros(pos.shape, f32)
    pull[...] = jnp.zeros(pull.shape, f32)
    for ref in placed:
        ref[...] = jnp.zeros(ref.shape, f32)
    for n in (3, 2, 1, 5, 4):
        loads_in[n].wait()

    moved = frac[...]
    weights = [
        outer_weight(1.0 + moved),
        inner_weight(moved),
        inner_weight(1.0 - moved),
        outer_weight(2.0 - moved),
    ]
    lane = lax.broadcasted_iota(jnp.int32, (1, run), 1)
    slot = lax.rem(lane, window)
    of_tile = lax.rem(lane // window, tiles)
    start_of = jnp.zeros((1, run), jnp.int32)
    offsets = []
    for t in range(tiles):
        z = base[2:3, t * run : (t + 1) * run]
        gap = z - z[0:1, 0:1]
        gap = jnp.where(gap > depth // 2, gap - depth, gap)
        gap = jnp.where(gap < -(depth // 2), gap + depth, gap)
        low = jnp.min(gap, axis=1, keepdims=True)
        offsets.append(gap - low)
        start_of = jnp.where(of_tile == t, z[0:1, 0:1] + low - 1, start_of)
    zmap = wrap(start_of + slot, depth).astype(f32)
    offset = jnp.concatenate(offsets, axis=1)
    reach_z = pick4(lax.broadcasted_iota(jnp.int32, (window, count), 0) - offset, [w[2:3] for w in weights])

    pairs = up(tiles, 2) // 2
    ends = edges[...]
    tail = jnp.bitwise_and(ends[0:1], run - 1)
    head = jnp.bitwise_and(ends[1:2], run - 1)
    group = lax.shift_right_logical(ends[0:1], run.bit_length() - 1)
    whole = base[...].astype(f32) + moved
    for t in range(tiles):
        pos[pl.ds(4 * t, 3), :] = whole[:, t * run : (t + 1) * run]
    for k in (0, 4):
        pull[pl.ds(k, 3), :] = rest[...]
    half_of = lax.broadcasted_iota(jnp.int32, (8, edge_count), 0) // 4
    mine = [group == 2 * p + half_of for p in range(pairs)]
    tables = [pos[pl.ds(8 * p, 8), :] for p in range(pairs)]
    pieces_of = []
    for k in range(0, edge_count, run):
        cols = slice(k, k + run)
        heads_at, tails_at = (jnp.broadcast_to(value[:, cols], (8, run)) for value in (head, tail))
        piece = jnp.zeros((8, run), f32)
        fronts = [jnp.take_along_axis(table, heads_at, axis=1) for table in tables]
        backs = [jnp.take_along_axis(table, tails_at, axis=1) for table in tables]
        for p in range(pairs):
            piece = jnp.where(mine[p][:, cols], fronts[p] - backs[p], piece)
        pieces_of.append(piece)
    diff = jnp.concatenate(pieces_of, axis=1)
    stretch = stiff[...].reshape(1, edge_count) * (diff - pull[...])
    terms = jnp.concatenate([jnp.where(mine[p], stretch, 0.0) for p in range(pairs)], axis=0)
    spot = lax.broadcasted_iota(jnp.int32, (run, edge_count), 0).astype(f32).astype(bf16)
    one, none = jnp.ones((), bf16), jnp.zeros((), bf16)
    heads, tails = (value.astype(f32).astype(bf16) for value in (head, tail))
    hot = jnp.where(spot == heads, one, jnp.where(spot == tails, -one, none))
    part = 8 * pairs
    summed = transposed_dot(halves(terms), hot)
    mem[...] = -(summed[0:part] + summed[part : 2 * part])

    def moments(r):
        totals = [None] * 4
        for q, c in enumerate(lattice_speeds):
            value = pops[pl.ds(q * own + r, 8), :]
            for k, sign in enumerate((1,) + c):
                if sign:
                    term = value if sign > 0 else -value
                    totals[k] = term if totals[k] is None else totals[k] + term
        for k in range(4):
            for i in range(0, 8, wy):
                mac[pl.ds(k * rows + plan.row((r + i) // wy, 0), wy), :] = totals[k][i : i + wy]

    def pack(n):
        cells, close = plan.edge[n], plan.near[n]
        for k in range(4):
            move(
                mac,
                [k * rows + plan.row(x, y) for x, y in cells],
                ms[n],
                [k * len(cells) + i for i in range(len(cells))],
            )
        for s, q in enumerate(plan.dirs[n]):
            first = 4 * len(cells) + s * len(close)
            move(pops, [q * own + x * wy + y for x, y in close], ms[n], [first + i for i in range(len(close))])
        ms[n][pl.ds(plan.macro_rows[n] - 1, 1), :] = zmap

    late = (0, 1, 6, 2, 3, 7)

    bx = base[0:1, :] - ix * wx - 1
    by = base[1:2, :] - iy * wy - 1
    i = lax.broadcasted_iota(jnp.int32, (px_ref.shape[0], 1), 0)
    px_ref[...] = pick4(i - 1 - bx, [w[0:1] for w in weights])
    i = lax.broadcasted_iota(jnp.int32, (h, 1), 0)
    y = jnp.where(i == h - 1, -1, jnp.where(i > wy + 1, -100, i))
    py = pick4(y - by, [w[1:2] for w in weights])
    big, small = [], []
    for c in range(3):
        for t in range(tiles):
            cols = slice(t * run, (t + 1) * run)
            block = reach_z[:, cols] * mem[pl.ds(4 * t + c, 1), :]
            rounded = block.astype(bf16).astype(f32)
            for out, value in ((big, rounded), (small, block - rounded)):
                out.append(jnp.concatenate([value if t == s else zeros for s in range(tiles)], axis=1))
    pad = [jnp.zeros((run - 3 * tiles * window, count), f32)]
    source = jnp.concatenate(big + pad + small + pad, axis=0).astype(bf16)

    def spread(spans):
        for a, n in spans:
            for k in range(a // h, (a + n) // h):
                plane[pl.ds(k * h, h), :] = px_ref[pl.ds(k, 1), :] * py
        flat = jnp.concatenate([plane[pl.ds(a, n), :] for a, n in spans], axis=0)
        size = flat.shape[0]
        value = transposed_dot(halves(flat), source)
        value = value[0:size] + value[size : 2 * size]
        value = value[:, 0:run] + value[:, run : 2 * run]
        done = 0
        for a, n in spans:
            comb[pl.ds(a, n), :] = value[done : done + n]
            done += n

    left, right = 3 * h, wx * h
    spread([(0, left), (right, 3 * h)])
    for n in range(4):
        move(comb, [plan.row(x, y) for x, y in plan.force[n]], fs[n], list(range(plan.force_rows[n])))
    loads_in[0].wait()
    ends_of = sorted({x * wy // 8 * 8 for x in (0, 1, wx - 1)})
    for r in ends_of:
        moments(r)
    for n in late:
        pack(n)

    greetings = 8 - sum(lead)

    @pl.when(greetings > 0)
    def _():
        pl.semaphore_wait(barrier, greetings)

    for n in range(8):
        back = sides.index((-sides[n][0], -sides[n][1]))
        slot_of = [i for i, g in enumerate(groups) if back in g][0]

        @pl.when(lead[n] == 0)
        def _():
            hail(ready.at[slot_of], n)

    for n in late:

        @pl.when(lead[n] == 0)
        def _():
            macro_copies[n].start()
            force_copies[n].start()

    for r in range(0, own, 8):
        if r not in ends_of:
            moments(r)
    for n in (4, 5):
        pack(n)

    for n in (5, 4):

        @pl.when(lead[n] == 0)
        def _():
            macro_copies[n].start()

    spread([(left, right - left)])
    for n in (4, 5):
        move(comb, [plan.row(x, y) for x, y in plan.force[n]], fs[n], list(range(plan.force_rows[n])))
    for n in (5, 4):

        @pl.when(lead[n] == 0)
        def _():
            force_copies[n].start()

    gap = wrap(lax.broadcasted_iota(jnp.int32, (depth, count), 0) - (base[2:3, :] - 1), depth)
    z_high, z_low = split(pick4(gap, [w[2:3] for w in weights]))
    for k, value in enumerate((z_high, z_high, z_low)):
        along[pl.ds(k * depth, depth), :] = value

    for i in (2, 3, 0, 1):

        @pl.when(led[i] > 0)
        def _():
            pl.semaphore_wait(ready.at[i], led[i])

        for n in groups[i]:

            @pl.when(lead[n] == 1)
            def _():
                force_copies[n].start()
                macro_copies[n].start()

    comp_of = lane // (window * tiles)
    comps_of = jnp.concatenate([comp_of] * 3, axis=1)

    def mark(ones, s, zrow):
        at = jnp.where(lax.broadcasted_iota(jnp.int32, (depth, run), 0).astype(f32) == zrow, 1.0, 0.0)
        if ones.shape[0] == depth:
            ones[:, pl.ds(s * run, run)] = at.astype(bf16)
            return
        for c in range(3):
            ones[pl.ds(c * depth, depth), pl.ds(s * run, run)] = jnp.where(comp_of == c, at, 0.0).astype(bf16)

    def take_macro(n):
        cells, close, d = plan.edge[n], plan.near[n], sides[n]
        for k in range(4):
            move(
                mr[n],
                [k * len(cells) + i for i in range(len(cells))],
                mac,
                [k * rows + plan.there(c, d) for c in cells],
            )
        return mr[n][pl.ds(plan.macro_rows[n] - 1, 1), :]

    def pop_row(n, q, cell):
        cells, close = plan.edge[n], plan.near[n]
        return 4 * len(cells) + plan.dirs[n].index(q) * len(close) + close.index(cell)

    keep = 1.0 - 1.0 / relax_time
    half = 1.0 - 0.5 / relax_time
    level_row = lax.broadcasted_iota(jnp.int32, (h, 1), 0)

    def population(q, x):
        c = lattice_speeds[q]
        if x < 0 or x >= wx:
            return edge_pops[pl.ds(q * h, h), :]
        value = pops[pl.ds(q * own + x * wy, h), :]
        if c[1] == 1:
            value = jnp.where(level_row == h - 1, mr[4][pl.ds(pop_row(4, q, (x, wy - 1)), 1), :], value)
        if c[1] == -1:
            value = jnp.where(level_row == wy, mr[5][pl.ds(pop_row(5, q, (x, 0)), 1), :], value)
        return value

    def collide(x):
        at = (x + 1) * h
        density = mac[pl.ds(at, h), :]
        force = [grid[pl.ds(k * rows + at, h), :] for k in range(3)]
        inverse = 1.0 / density
        speed = [(mac[pl.ds((k + 1) * rows + at, h), :] + 0.5 * force[k]) * inverse for k in range(3)]
        for k in range(3):
            held = jnp.where((level_row <= wy + 1) | (level_row == h - 1), speed[k], 0.0)
            vel[pl.ds(k * rows + at, h), :] = held
        square = speed[0] * speed[0] + speed[1] * speed[1] + speed[2] * speed[2]
        work = speed[0] * force[0] + speed[1] * force[1] + speed[2] * force[2]
        scaled = density * (1.0 / relax_time)
        level = scaled * (1.0 - 1.5 * square) - (3.0 * half) * work
        carried = [scaled * speed[k] for k in range(3)]
        pushed = [half * force[k] for k in range(3)]
        odd_of = [carried[k] + pushed[k] for k in range(3)]
        even_of = [odd_of[k] + pushed[k] for k in range(3)]
        levels, odds, evens = {}, {}, {}
        for weight in sorted({lattice_weights[q] for q in range(19)}):
            levels[weight] = weight * level
            odds[weight] = [(3.0 * weight) * odd_of[k] for k in range(3)]
            evens[weight] = [(4.5 * weight) * even_of[k] for k in range(3)]
        for first in [0] + list(range(1, 19, 2)):
            pair = [0] if first == 0 else [first, first + 1]
            pair = [q for q in pair if 0 <= x + lattice_speeds[q][0] < wx]
            if not pair:
                continue
            weight = lattice_weights[first]
            even, odd = levels[weight], None
            if first:
                c = lattice_speeds[first]
                even = even + along_speed(c, speed) * along_speed(c, evens[weight])
                odd = along_speed(c, odds[weight])
            for q in pair:
                c = lattice_speeds[q]
                total = even if odd is None else even + odd if q == first else even - odd
                value = keep * population(q, x) + total
                if c[1]:
                    value = pltpu.roll(value, c[1] % h, 0)
                if c[2]:
                    value = pltpu.roll(value, c[2] % depth, 1)
                fresh[pl.ds(q * own + (x + c[0]) * wy, wy), :] = value[0:wy]

    mark(ones_y, 0, zmap)
    arrive(1, (4, 5))
    for s, n in ((1, 4), (2, 5)):
        mark(ones_y, s, take_macro(n))
    arrive(3, (4, 5))
    for n in (4, 5):
        move(fr[n], list(range(plan.force_rows[n])), placed[n], [plan.there(c, sides[n]) for c in plan.force[n]])

    def widen(parts, ones):
        value = transposed_dot(halves(jnp.concatenate(parts, axis=1)), ones[...])
        half_rows = value.shape[0] // 2
        return value[0:half_rows] + value[half_rows:]

    value = widen([comb[...], placed[4][...], placed[5][...]], ones_y)
    for c in range(3):
        grid[pl.ds(c * rows, rows), :] = value[:, c * depth : (c + 1) * depth]
    for x in plan.xs:
        if not plan.late(x):
            collide(x)

    for k, value in enumerate(sample(vel, plane, along, rows, [(left, right - left)])):
        part_sum[pl.ds(8 * k, 8), :] = value

    arrive(1, late)
    for ones, order in ((ones_l, (6, 0, 1)), (ones_r, (7, 2, 3))):
        for s, n in enumerate(order):
            mark(ones, s, take_macro(n))
            for q in plan.dirs[n]:
                close = plan.near[n]
                src = [pop_row(n, q, c) for c in close]
                move(mr[n], src, edge_pops, [q * h + (c[1] - sides[n][1] * wy) % h for c in close])
    arrive(3, late)
    for ones, order, at in ((ones_l, (6, 0, 1), 0), (ones_r, (7, 2, 3), right)):
        for n in order[1:]:
            dst = [plan.there(c, sides[n]) - at for c in plan.force[n]]
            move(fr[n], list(range(plan.force_rows[n])), placed[n], dst)
        parts = jnp.concatenate([fr[order[0]][...], placed[order[1]][...], placed[order[2]][...]], axis=1)
        rounded = parts.astype(bf16).astype(f32)
        both = (rounded, parts - rounded)
        parts = jnp.concatenate([jnp.where(comps_of == c, value, 0.0) for value in both for c in range(3)], axis=0)
        value = transposed_dot(parts.astype(bf16), ones[...])
        for c in range(3):
            here = pl.ds(c * rows + at, 3 * h)
            both = value[3 * h * c : 3 * h * (c + 1)] + value[3 * h * (c + 3) : 3 * h * (c + 4)]
            grid[here, :] = grid[here, :] + both
    for x in plan.xs:
        if plan.late(x):
            collide(x)
    sent = pops.at[pl.ds(0, sum(plan.macro_rows) + sum(plan.force_rows)), :]
    pltpu.make_async_remote_copy(
        src_ref=sent,
        dst_ref=sent,
        send_sem=sems.at[0],
        recv_sem=sems.at[1],
        device_id=peers[0],
        device_id_type=pl.DeviceIdType.MESH,
    ).wait_send()


def finish_kernel(plan, fresh, vel, plane, along, part_sum, fresh_out, sampled_out, sampled, sems):
    h, size = plan.h, fresh.shape[0]
    step = up(size // pieces, 8)
    leave = []
    for i in range(pieces):
        here = pl.ds(i * step, min(step, size - i * step))
        leave.append(pltpu.make_async_copy(fresh.at[here, :], fresh_out.at[here, :], sems.at[i]))
    for copy in leave:
        copy.start()
    leave.append(pltpu.make_async_copy(sampled, sampled_out, sems.at[pieces]))
    for k, value in enumerate(sample(vel, plane, along, plan.rows, [(0, 3 * h), (plan.wx * h, 3 * h)])):
        value = value + part_sum[pl.ds(8 * k, 8), :]
        sampled[k : k + 1, :] = jnp.sum(value, axis=0, keepdims=True)
    leave[-1].start()
    for copy in leave:
        copy.wait()


def solution(mesh):
    nx, ny = mesh.shape["gx"], mesh.shape["gy"]

    def per_device(populations, vert_base, vert_frac, edges, stiffness, rest):
        _, wx, wy, depth = populations.shape
        count, edge_count = vert_base.shape[1], edges.shape[1]
        plan = Plan(wx, wy)
        rows, tiles, h = plan.rows, count // run, plan.h
        macro = [pltpu.VMEM((n, depth), f32) for n in plan.macro_rows]
        force = [pltpu.VMEM((n, run), f32) for n in plan.force_rows]
        scratch = macro + macro + force + force
        scratch += [
            pltpu.VMEM((19 * wx * wy + h, depth), f32),
            pltpu.VMEM((3, count), jnp.int32),
            pltpu.VMEM((3, count), f32),
            pltpu.VMEM((2, edge_count), jnp.int32),
            pltpu.VMEM((edge_count,), f32),
            pltpu.VMEM((3, edge_count), f32),
            pltpu.VMEM((up(4 * tiles, 8), run), f32),
            pltpu.VMEM((8, edge_count), f32),
            pltpu.VMEM((up(4 * tiles, 8), run), f32),
            pltpu.VMEM((4 * rows, depth), f32),
            pltpu.VMEM((3 * rows, depth), f32),
            pltpu.VMEM((rows, run), f32),
            pltpu.VMEM((up(plan.cols, 8), count), f32),
        ]
        scratch += [pltpu.VMEM((rows if n in (4, 5) else 3 * h, run), f32) for n in range(8)]
        scratch += [pltpu.VMEM((n * depth, 3 * run), bf16) for n in (3, 1, 1)]
        scratch += [
            pltpu.VMEM((19 * h, depth), f32),
            pltpu.SemaphoreType.DMA((5,)),
            pltpu.SemaphoreType.DMA((2,)),
            pltpu.SemaphoreType.REGULAR((len(groups),)),
        ]
        vmem = pl.BlockSpec(memory_space=pltpu.VMEM)
        far = pl.BlockSpec(memory_space=pltpu.HBM)

        def exchange(*refs):
            exchange_kernel(plan, nx, ny, *refs)

        def finish(*refs):
            finish_kernel(plan, *refs)

        held = pl.pallas_call(
            exchange,
            out_shape=(
                jax.ShapeDtypeStruct((19 * wx * wy, depth), f32),
                jax.ShapeDtypeStruct((3 * rows, depth), f32),
                jax.ShapeDtypeStruct((rows, count), f32),
                jax.ShapeDtypeStruct((3 * depth, count), bf16),
                jax.ShapeDtypeStruct((24, count), f32),
            ),
            in_specs=[far] * 6,
            out_specs=(vmem,) * 5,
            scratch_shapes=scratch,
            compiler_params=pltpu.CompilerParams(
                collective_id=0, has_side_effects=True, vmem_limit_bytes=24 * 1024 * 1024
            ),
            name="exchange",
        )(
            *[
                pltpu.with_memory_space_constraint(value, pltpu.HBM)
                for value in (
                    populations.reshape(19 * wx * wy, depth),
                    vert_base,
                    vert_frac,
                    edges,
                    stiffness,
                    rest,
                )
            ]
        )
        fresh, sampled = pl.pallas_call(
            finish,
            out_shape=(
                jax.ShapeDtypeStruct((19 * wx * wy, depth), f32),
                jax.ShapeDtypeStruct((3, count), f32),
            ),
            in_specs=[vmem] * 5,
            out_specs=(far, far),
            scratch_shapes=[pltpu.VMEM((3, count), f32), pltpu.SemaphoreType.DMA((pieces + 1,))],
            compiler_params=pltpu.CompilerParams(vmem_limit_bytes=24 * 1024 * 1024),
            name="finish",
        )(*held)
        return fresh.reshape(19, wx, wy, depth), sampled

    placed = (
        P(None, "gx", "gy", None),
        P(None, ("gx", "gy")),
        P(None, ("gx", "gy")),
        P(None, ("gx", "gy")),
        P(("gx", "gy")),
        P(None, ("gx", "gy")),
    )
    return jax.shard_map(
        per_device,
        mesh=mesh,
        in_specs=placed,
        out_specs=(P(None, "gx", "gy", None), P(None, ("gx", "gy"))),
        check_vma=False,
    )
```
